32 devices in a mesh: lat: 4 (over x, core), lon: 2 (over y), lev: 4 (over z).
Axes of the slice: x: 2, y: 2, z: 4, core: 2. Of those that a mesh axis runs over, the one named last changes fastest.
Arguments:
- outer_increment: bfloat16 [16, 256, 1024], P('lev', 'lat', 'lon'), may hold values from -6 to 6
- courant: bfloat16 [3, 16, 64, 256], P(None, 'lev', 'lat', 'lon'), may hold values from -0.29882812 to 0.29882812
- obs_column: int32 [16384], P(('lat', 'lon')), may hold values from 0 to 2047
- obs_level: int32 [16384], P(('lat', 'lon')), may hold values from 0 to 15
- obs_value: float32 [16384], P(('lat', 'lon')), may hold values from -6 to 6
Outputs:
- inner_state: float32 [16, 64, 256], P('lev', 'lat', 'lon')
- adjoint: float32 [16, 64, 256], P('lev', 'lat', 'lon')
- outer_next: bfloat16 [16, 256, 1024], P('lev', 'lat', 'lon')
The draws below stay inside these ranges and needn't reach their ends.
Inputs may be any that keep to these rules, and one draw needn't show every extreme that they name: obs_column numbers a column of the 16 x 512 / 4 inner block of its latitude-longitude block, row by row.
All inputs are finite; a program needn't handle non-finite values.
Results may differ from the reference program's by a relative error of at most 0.001.
Values sent between devices are 32-bit elements; how exact they have to be, the bound alone decides.
A program may use at most 64 MiB of HBM per device.

```python
import jax
import jax.numpy as jnp

CLAT = 64
CLON = 512
OBS_COL = 2048
NLAT = 256
NLON = 1024
NLEV = 16
NOBS = 16384
N_LON = 2


def with_ends(drawn, rng, low, top_value):
    index_at = [jax.random.randint(jax.random.fold_in(rng, axis), (), 0, length) for axis, length in enumerate(drawn.shape)]
    widest = drawn.shape.index(max(drawn.shape))
    neighbour = index_at[:widest] + [(index_at[widest] + 1) % drawn.shape[widest]] + index_at[widest + 1:]
    return drawn.at[tuple(index_at)].set(low).at[tuple(neighbour)].set(top_value)


def block_levels(rng, extent, shards, smallest, high):
    gain = 1.0
    for dim, blocks in shards:
        draws = jax.random.uniform(jax.random.fold_in(jax.random.fold_in(rng, 6), dim), (blocks,), jnp.float32, smallest / len(shards), high / len(shards))
        gain = gain * jnp.repeat(jnp.exp(draws), extent[dim] // blocks).reshape((-1,) + (1,) * (len(extent) - 1 - dim))
    return gain


def noise(rng, shape, scale, limit, pieces=(), kind=jnp.bfloat16):
    entries = jax.random.normal(rng, shape, jnp.float32) * scale
    if len(pieces) > 0:
        entries = block_levels(rng, shape, pieces, -0.22, 0.18) * entries
    return jnp.clip(entries, min=-limit, max=limit).astype(kind)


def setup_inputs(seed: int = 0) -> dict:
    keys = jax.random.split(jax.random.key(seed), 6)
    outer_increment = noise(keys[0], (NLEV, NLAT, NLON), 1.0, 6.0, ((0, 4), (1, 4), (2, 2)))
    courant = jnp.clip(jax.random.uniform(keys[1], (3, NLEV, NLAT // 4, NLON // 4), jnp.float32, -0.29882812, 0.29882812) * block_levels(keys[1], (3, NLEV, NLAT // 4, NLON // 4), ((1, 4), (2, 4), (3, 2)), -0.4, 0.0), -0.29882812, 0.29882812).astype(jnp.bfloat16)
    obs_column = with_ends(jax.random.randint(keys[2], (NOBS,), 0, CLAT * CLON // 16), jax.random.fold_in(keys[2], 1), 0, (CLAT * CLON // 16) - 1).astype(jnp.int32)
    obs_level = with_ends(jax.random.randint(keys[3], (NOBS,), 0, NLEV), jax.random.fold_in(keys[3], 1), 0, NLEV - 1).astype(jnp.int32)
    obs_value = noise(keys[4], (NOBS,), 1.0, 6.0, ((0, 8),), jnp.float32)
    return {"outer_increment": outer_increment, "courant": courant, "obs_column": obs_column, "obs_level": obs_level, "obs_value": obs_value}


def extend(field):
    wrapped = jnp.pad(field, ((0, 0), (0, 0), (0, 0), (1, 1)), mode="wrap")
    return jnp.pad(wrapped, ((0, 0), (1, 1), (1, 1), (0, 0)))


def window_of(field, axis, shift):
    sizes = [field.shape[1] - 2, field.shape[2] - 2, field.shape[3] - 2]
    begins = [1, 1, 1]
    begins[axis - 1] = begins[axis - 1] + shift
    return field[:, begins[0]:begins[0] + sizes[0], begins[1]:begins[1] + sizes[1], begins[2]:begins[2] + sizes[2]]


def forward(state, rims_courant):
    numbers = window_of(rims_courant, 1, 0)
    result = (1.0 - jnp.sum(jnp.abs(numbers), axis=0, keepdims=True)) * state
    padded = extend(state)
    for direction in range(3):
        lower = jnp.maximum(numbers[direction:direction + 1], 0.0)
        upper = jnp.maximum(-numbers[direction:direction + 1], 0.0)
        result = result + lower * window_of(padded, direction + 1, -1) + upper * window_of(padded, direction + 1, 1)
    return result


def backward(adjoint, rims_courant):
    numbers = window_of(rims_courant, 1, 0)
    result = (1.0 - jnp.sum(jnp.abs(numbers), axis=0, keepdims=True)) * adjoint
    padded = extend(adjoint)
    for direction in range(3):
        lower = jnp.maximum(rims_courant[direction:direction + 1], 0.0)
        upper = jnp.maximum(-rims_courant[direction:direction + 1], 0.0)
        result = result + window_of(lower * padded, direction + 1, 1) + window_of(upper * padded, direction + 1, -1)
    return result


def reference(outer_increment, courant, obs_column, obs_level, obs_value):
    levels, rows, columns = outer_increment.shape
    inner_rows = rows // 4
    inner_cols = columns // 4
    blocked = outer_increment.reshape(levels, inner_rows, 4, inner_cols, 4)
    coarse = jnp.mean(blocked, axis=(2, 4), dtype=jnp.float32).astype(jnp.float32)
    rims_courant = extend(courant.astype(jnp.float32))
    state = coarse[None]
    for turn in range(2):
        state = forward(state, rims_courant)
    block_rows = CLAT // 4
    block_cols = CLON // 4
    blocks = jnp.arange(obs_column.shape[0], dtype=jnp.int32) // OBS_COL
    row_index = (blocks // N_LON) * block_rows + obs_column // block_cols
    col_index = (blocks % N_LON) * block_cols + obs_column % block_cols
    flat = ((obs_level * inner_rows + row_index) * inner_cols + col_index).astype(jnp.int32)
    innovation = state.reshape(-1)[flat] - obs_value
    forcing = jnp.zeros((levels * inner_rows * inner_cols,), jnp.float32).at[flat].add(innovation)
    adjoint = forcing.reshape(1, levels, inner_rows, inner_cols)
    for turn in range(2):
        adjoint = backward(adjoint, rims_courant)
    spread = jnp.broadcast_to(adjoint[0][:, :, None, :, None], (levels, inner_rows, 4, inner_cols, 4)).reshape(levels, rows, columns)
    outer_next = (outer_increment.astype(jnp.float32) - spread).astype(jnp.bfloat16)
    return state[0], adjoint[0], outer_next
```

```python
import functools

import jax
import jax.numpy as jnp
from jax import lax
from jax.experimental import pallas as pl
from jax.experimental.pallas import tpu as pltpu
from jax.sharding import PartitionSpec as P

MESH = pl.DeviceIdType.MESH
ROUNDS = 4


def bf16_parts(x, count):
    parts = []
    for _ in range(count):
        part = x.astype(jnp.bfloat16).astype(jnp.float32)
        parts.append(part)
        x = x - part
    return parts


def kernel(
    ends, outer_hbm, courant_hbm, col_hbm, lvl_hbm, val_hbm,
    state_hbm, adj_hbm, next_hbm,
    outer, courant, col, lvl, val, sums, wide, nxt, state_v, adj_v,
    lev_out, lat_out, lon_out, lev_in, lat_in, lon_in,
    in_sem, out_sem, send_sem, recv_sem,
):
    n_lat, n_lon, n_lev = ends
    levels, rows, cols = state_v.shape
    flat_rows = levels * rows
    wide_cols = outer.shape[1]
    fine = wide_cols // cols
    outer_rows = outer.shape[0] // levels

    loads = [
        pltpu.make_async_copy(src, dst, in_sem.at[i])
        for i, (src, dst) in enumerate(
            ((outer_hbm, outer), (courant_hbm, courant), (col_hbm, col), (lvl_hbm, lvl), (val_hbm, val))
        )
    ]
    for load in loads:
        load.start()

    me_lat, me_lon, me_lev = (lax.axis_index(a) for a in ("lat", "lon", "lev"))
    links = (
        ("lev", me_lev + 1, me_lev < n_lev - 1),
        ("lev", me_lev - 1, me_lev > 0),
        ("lat", me_lat + 1, me_lat < n_lat - 1),
        ("lat", me_lat - 1, me_lat > 0),
        ("lon", lax.rem(me_lon + 1, n_lon), None),
        ("lon", lax.rem(me_lon + n_lon - 1, n_lon), None),
    )
    outs = {"lev": lev_out, "lat": lat_out, "lon": lon_out}
    ins = {"lev": lev_in, "lat": lat_in, "lon": lon_in}

    def guarded(exists, action):
        if exists is None:
            action()
        else:
            pl.when(exists)(action)

    barrier = pltpu.get_barrier_semaphore()
    for axis, who, exists in links:
        guarded(
            exists,
            lambda axis=axis, who=who: pl.semaphore_signal(
                barrier, inc=1, device_id={axis: who}, device_id_type=MESH
            ),
        )

    def message(turn, which):
        axis, who, _ = links[which]
        side = which % 2
        source = outs[axis].at[turn] if axis == "lon" else outs[axis].at[turn, side]
        return pltpu.make_async_remote_copy(
            src_ref=source,
            dst_ref=ins[axis].at[turn, side],
            send_sem=send_sem.at[turn, which],
            recv_sem=recv_sem.at[turn, which],
            device_id={axis: who},
            device_id_type=MESH,
        )

    def blank(ref, side):
        for turn in range(ROUNDS):
            ref[turn, side] = jnp.zeros(ref.shape[2:], jnp.float32)

    pl.when(me_lev == 0)(lambda: blank(lev_in, 0))
    pl.when(me_lev == n_lev - 1)(lambda: blank(lev_in, 1))
    pl.when(me_lat == 0)(lambda: blank(lat_in, 0))
    pl.when(me_lat == n_lat - 1)(lambda: blank(lat_in, 1))

    lane = lax.broadcasted_iota(jnp.int32, (flat_rows, cols), 1)
    flat = lax.broadcasted_iota(jnp.int32, (flat_rows, cols), 0)
    lane3 = lax.broadcasted_iota(jnp.int32, (levels, rows, cols), 2)
    row3 = lax.broadcasted_iota(jnp.int32, (levels, rows, cols), 1)

    pool = (
        lax.broadcasted_iota(jnp.int32, (wide_cols, cols), 0) // fine
        == lax.broadcasted_iota(jnp.int32, (wide_cols, cols), 1)
    ).astype(jnp.float32).astype(jnp.bfloat16)

    loads[0].wait()
    sums[...] = jnp.dot(outer[...], pool, preferred_element_type=jnp.float32)
    coarse = sums[pl.ds(0, flat_rows, stride=fine), :]
    for k in range(1, fine):
        coarse = coarse + sums[pl.ds(k, flat_rows, stride=fine), :]
    coarse = (coarse * (1.0 / (fine * fine))).reshape(levels, rows, cols)

    def send(turn, firsts, lasts):
        lev_out[turn, 0] = lasts[0][levels - 1]
        lev_out[turn, 1] = firsts[0][0]
        lat_out[turn, 0] = lasts[1][:, rows - 1, :]
        lat_out[turn, 1] = firsts[1][:, 0, :]
        for which in range(4):
            guarded(links[which][2], lambda which=which: message(turn, which).start())
        first = firsts[2].reshape(flat_rows, cols)[:, :1]
        last = lasts[2].reshape(flat_rows, cols)[:, cols - 1 :]
        spread = jnp.where(lane == flat, first, 0.0) + jnp.where(lane == flat + flat_rows, last, 0.0)
        lon_out[turn] = jnp.sum(spread, axis=0, keepdims=True)
        for which in (4, 5):
            message(turn, which).start()

    def receive(turn, firsts, lasts):
        for which in range(4):
            guarded(links[which ^ 1][2], lambda which=which: message(turn, which).wait_recv())
        below = [
            jnp.concatenate([lev_in[turn, 0][None], lasts[0][: levels - 1]], axis=0),
            jnp.where(row3 == 0, lat_in[turn, 0][:, None, :], pltpu.roll(lasts[1], 1, axis=1)),
        ]
        above = [
            jnp.concatenate([firsts[0][1:], lev_in[turn, 1][None]], axis=0),
            jnp.where(row3 == rows - 1, lat_in[turn, 1][:, None, :], pltpu.roll(firsts[1], rows - 1, axis=1)),
        ]
        for which in (4, 5):
            message(turn, which).wait_recv()
        left = jnp.sum(
            jnp.where(lane == flat + flat_rows, lon_in[turn, 0], 0.0), axis=1, keepdims=True
        ).reshape(levels, rows, 1)
        right = jnp.sum(jnp.where(lane == flat, lon_in[turn, 1], 0.0), axis=1, keepdims=True).reshape(
            levels, rows, 1
        )
        below.append(jnp.where(lane3 == 0, left, pltpu.roll(lasts[2], 1, axis=2)))
        above.append(jnp.where(lane3 == cols - 1, right, pltpu.roll(firsts[2], cols - 1, axis=2)))
        return below, above

    expected = sum(1 if e is None else e.astype(jnp.int32) for _, _, e in links)
    pl.semaphore_wait(barrier, expected)
    send(0, [coarse] * 3, [coarse] * 3)

    loads[1].wait()
    numbers = courant[...].astype(jnp.float32)
    lower = [jnp.maximum(numbers[k], 0.0) for k in range(3)]
    upper = [jnp.maximum(-numbers[k], 0.0) for k in range(3)]
    centre = 1.0 - jnp.abs(numbers[0]) - jnp.abs(numbers[1]) - jnp.abs(numbers[2])

    for load in loads[2:]:
        load.wait()
    where_row = (lvl[...] - me_lev * levels) * rows + col[...] // cols
    where_col = col[...] % cols
    parts = bf16_parts(val[...], 3)
    pieces, width = col.shape
    row_id = lax.broadcasted_iota(jnp.int32, (flat_rows, width), 0)
    col_id = lax.broadcasted_iota(jnp.int32, (cols, width), 0)
    hits = [[] for _ in range(4)]
    tables = []
    for k in range(pieces):
        match = where_row[k : k + 1] == row_id
        hits[0].append(jnp.where(match, 1.0, 0.0).astype(jnp.bfloat16))
        for i, part in enumerate(parts):
            hits[i + 1].append(jnp.where(match, part[k : k + 1], 0.0).astype(jnp.bfloat16))
        tables.append(jnp.where(where_col[k : k + 1] == col_id, 1.0, 0.0).astype(jnp.bfloat16))
    left_side = jnp.concatenate([jnp.concatenate(h, axis=1) for h in hits], axis=0)
    totals = lax.dot_general(
        left_side, jnp.concatenate(tables, axis=1), (((1,), (1,)), ((), ())),
        preferred_element_type=jnp.float32,
    )
    count = totals[:flat_rows].reshape(levels, rows, cols)
    observed = (
        totals[flat_rows : 2 * flat_rows]
        + totals[2 * flat_rows : 3 * flat_rows]
        + totals[3 * flat_rows :]
    ).reshape(levels, rows, cols)

    def forward(field, turn):
        below, above = receive(turn, [field] * 3, [field] * 3)
        result = centre * field
        for k in range(3):
            result = result + lower[k] * below[k] + upper[k] * above[k]
        return result

    state = forward(coarse, 0)
    send(1, [state] * 3, [state] * 3)
    state = forward(state, 1)
    field = count * state - observed

    for turn in (2, 3):
        firsts = [lower[k] * field for k in range(3)]
        lasts = [upper[k] * field for k in range(3)]
        send(turn, firsts, lasts)
        if turn == 2:
            state_v[...] = state
            store_state = pltpu.make_async_copy(state_v, state_hbm, out_sem.at[0])
            store_state.start()
        below, above = receive(turn, firsts, lasts)
        result = centre * field
        for k in range(3):
            result = result + above[k] + below[k]
        field = result
    adj_v[...] = field
    store_adj = pltpu.make_async_copy(adj_v, adj_hbm, out_sem.at[1])
    store_adj.start()

    table = (
        lax.broadcasted_iota(jnp.int32, (cols, wide_cols), 0)
        == lax.broadcasted_iota(jnp.int32, (cols, wide_cols), 1) // fine
    ).astype(jnp.float32).astype(jnp.bfloat16)
    halves = bf16_parts(field.reshape(flat_rows, cols), 2)
    spread = jnp.dot(
        jnp.concatenate([h.astype(jnp.bfloat16) for h in halves], axis=1),
        jnp.concatenate([table, table], axis=0),
        preferred_element_type=jnp.float32,
    )
    for k in range(fine):
        for c in range(fine):
            span = pl.ds(c * cols, cols)
            wide[c, pl.ds(k, flat_rows, stride=fine), :] = spread[:, c * cols : (c + 1) * cols]
    stores = []
    for level in range(levels):
        span = pl.ds(level * outer_rows, outer_rows)
        for c in range(fine):
            lanes = pl.ds(c * cols, cols)
            nxt[span, lanes] = (outer[span, lanes].astype(jnp.float32) - wide[c, span, :]).astype(jnp.bfloat16)
        store = pltpu.make_async_copy(nxt.at[span], next_hbm.at[span], out_sem.at[2 + level])
        store.start()
        stores.append(store)

    for turn in range(ROUNDS):
        for which in range(6):
            guarded(links[which][2], lambda turn=turn, which=which: message(turn, which).wait_send())
    for store in [store_state, store_adj] + stores:
        store.wait()


def shards(ends, outer_increment, courant, obs_column, obs_level, obs_value):
    levels, outer_rows, wide_cols = outer_increment.shape
    _, _, rows, cols = courant.shape
    flat_rows = levels * rows
    fine = wide_cols // cols
    lanes = 128
    observed = (obs_column.shape[0] // lanes, lanes)
    assert 2 * flat_rows <= cols
    f32, bf16 = jnp.float32, jnp.bfloat16
    state, adjoint, following = pl.pallas_call(
        functools.partial(kernel, ends),
        out_shape=(
            jax.ShapeDtypeStruct((levels, rows, cols), f32),
            jax.ShapeDtypeStruct((levels, rows, cols), f32),
            jax.ShapeDtypeStruct((levels * outer_rows, wide_cols), bf16),
        ),
        in_specs=[pl.BlockSpec(memory_space=pl.ANY)] * 5,
        out_specs=(pl.BlockSpec(memory_space=pl.ANY),) * 3,
        scratch_shapes=[
            pltpu.VMEM((levels * outer_rows, wide_cols), bf16),
            pltpu.VMEM(courant.shape, bf16),
            pltpu.VMEM(observed, jnp.int32),
            pltpu.VMEM(observed, jnp.int32),
            pltpu.VMEM(observed, f32),
            pltpu.VMEM((levels * outer_rows, cols), f32),
            pltpu.VMEM((fine, levels * outer_rows, cols), f32),
            pltpu.VMEM((levels * outer_rows, wide_cols), bf16),
            pltpu.VMEM((levels, rows, cols), f32),
            pltpu.VMEM((levels, rows, cols), f32),
            pltpu.VMEM((ROUNDS, 2, rows, cols), f32),
            pltpu.VMEM((ROUNDS, 2, levels, cols), f32),
            pltpu.VMEM((ROUNDS, 1, cols), f32),
            pltpu.VMEM((ROUNDS, 2, rows, cols), f32),
            pltpu.VMEM((ROUNDS, 2, levels, cols), f32),
            pltpu.VMEM((ROUNDS, 2, 1, cols), f32),
            pltpu.SemaphoreType.DMA((5,)),
            pltpu.SemaphoreType.DMA((2 + levels,)),
            pltpu.SemaphoreType.DMA((ROUNDS, 6)),
            pltpu.SemaphoreType.DMA((ROUNDS, 6)),
        ],
        compiler_params=pltpu.CompilerParams(collective_id=0, has_side_effects=True),
    )(
        outer_increment.reshape(levels * outer_rows, wide_cols),
        courant,
        obs_column.reshape(observed),
        obs_level.reshape(observed),
        obs_value.reshape(observed),
    )
    return state, adjoint, following.reshape(outer_increment.shape)


def solution(mesh):
    ends = tuple(mesh.shape[a] for a in ("lat", "lon", "lev"))
    block = P("lev", "lat", "lon")
    observed = P(("lat", "lon"))
    return jax.shard_map(
        functools.partial(shards, ends),
        mesh=mesh,
        in_specs=(block, P(None, "lev", "lat", "lon"), observed, observed, observed),
        out_specs=(block, block, block),
        check_vma=False,
    )
```

```python
import functools

import jax
import jax.numpy as jnp
from jax import lax
from jax.experimental import pallas as pl
from jax.experimental.pallas import tpu as pltpu
from jax.sharding import PartitionSpec as P

MESH = pl.DeviceIdType.MESH
ROUNDS = 4


def bf16_parts(x, count):
    parts = []
    for _ in range(count):
        part = x.astype(jnp.bfloat16).astype(jnp.float32)
        parts.append(part)
        x = x - part
    return parts


def kernel(
    ends, outer_hbm, courant_hbm, col_hbm, lvl_hbm, val_hbm,
    state_v, adj_v, outer,
    courant, col, lvl, val, sums,
    lev_out, lat_out, lon_out, lev_in, lat_in, lon_in,
    in_sem, send_sem, recv_sem,
):
    n_lat, n_lon, n_lev = ends
    levels, rows, cols = state_v.shape
    flat_rows = levels * rows
    wide_cols = outer.shape[1]
    fine = wide_cols // cols

    loads = [
        pltpu.make_async_copy(src, dst, in_sem.at[i])
        for i, (src, dst) in enumerate(
            ((outer_hbm, outer), (courant_hbm, courant), (col_hbm, col), (lvl_hbm, lvl), (val_hbm, val))
        )
    ]
    for load in loads:
        load.start()

    me_lat, me_lon, me_lev = (lax.axis_index(a) for a in ("lat", "lon", "lev"))
    links = (
        ("lev", me_lev + 1, me_lev < n_lev - 1),
        ("lev", me_lev - 1, me_lev > 0),
        ("lat", me_lat + 1, me_lat < n_lat - 1),
        ("lat", me_lat - 1, me_lat > 0),
        ("lon", lax.rem(me_lon + 1, n_lon), None),
        ("lon", lax.rem(me_lon + n_lon - 1, n_lon), None),
    )
    outs = {"lev": lev_out, "lat": lat_out, "lon": lon_out}
    ins = {"lev": lev_in, "lat": lat_in, "lon": lon_in}

    def guarded(exists, action):
        if exists is None:
            action()
        else:
            pl.when(exists)(action)

    barrier = pltpu.get_barrier_semaphore()
    for axis, who, exists in links:
        guarded(
            exists,
            lambda axis=axis, who=who: pl.semaphore_signal(
                barrier, inc=1, device_id={axis: who}, device_id_type=MESH
            ),
        )

    def message(turn, which):
        axis, who, _ = links[which]
        side = which % 2
        source = outs[axis].at[turn] if axis == "lon" else outs[axis].at[turn, side]
        return pltpu.make_async_remote_copy(
            src_ref=source,
            dst_ref=ins[axis].at[turn, side],
            send_sem=send_sem.at[turn, which],
            recv_sem=recv_sem.at[turn, which],
            device_id={axis: who},
            device_id_type=MESH,
        )

    def blank(ref, side):
        for turn in range(ROUNDS):
            ref[turn, side] = jnp.zeros(ref.shape[2:], jnp.float32)

    pl.when(me_lev == 0)(lambda: blank(lev_in, 0))
    pl.when(me_lev == n_lev - 1)(lambda: blank(lev_in, 1))
    pl.when(me_lat == 0)(lambda: blank(lat_in, 0))
    pl.when(me_lat == n_lat - 1)(lambda: blank(lat_in, 1))

    lane = lax.broadcasted_iota(jnp.int32, (flat_rows, cols), 1)
    flat = lax.broadcasted_iota(jnp.int32, (flat_rows, cols), 0)
    lane3 = lax.broadcasted_iota(jnp.int32, (levels, rows, cols), 2)
    row3 = lax.broadcasted_iota(jnp.int32, (levels, rows, cols), 1)

    pool = (
        lax.broadcasted_iota(jnp.int32, (wide_cols, cols), 0) // fine
        == lax.broadcasted_iota(jnp.int32, (wide_cols, cols), 1)
    ).astype(jnp.float32).astype(jnp.bfloat16)

    loads[0].wait()
    sums[...] = jnp.dot(outer[...], pool, preferred_element_type=jnp.float32)
    coarse = sums[pl.ds(0, flat_rows, stride=fine), :]
    for k in range(1, fine):
        coarse = coarse + sums[pl.ds(k, flat_rows, stride=fine), :]
    coarse = (coarse * (1.0 / (fine * fine))).reshape(levels, rows, cols)

    def send(turn, firsts, lasts):
        lev_out[turn, 0] = lasts[0][levels - 1]
        lev_out[turn, 1] = firsts[0][0]
        lat_out[turn, 0] = lasts[1][:, rows - 1, :]
        lat_out[turn, 1] = firsts[1][:, 0, :]
        for which in range(4):
            guarded(links[which][2], lambda which=which: message(turn, which).start())
        first = firsts[2].reshape(flat_rows, cols)[:, :1]
        last = lasts[2].reshape(flat_rows, cols)[:, cols - 1 :]
        spread = jnp.where(lane == flat, first, 0.0) + jnp.where(lane == flat + flat_rows, last, 0.0)
        lon_out[turn] = jnp.sum(spread, axis=0, keepdims=True)
        for which in (4, 5):
            message(turn, which).start()

    def receive(turn, firsts, lasts):
        for which in range(4):
            guarded(links[which ^ 1][2], lambda which=which: message(turn, which).wait_recv())
        below = [
            jnp.concatenate([lev_in[turn, 0][None], lasts[0][: levels - 1]], axis=0),
            jnp.where(row3 == 0, lat_in[turn, 0][:, None, :], pltpu.roll(lasts[1], 1, axis=1)),
        ]
        above = [
            jnp.concatenate([firsts[0][1:], lev_in[turn, 1][None]], axis=0),
            jnp.where(row3 == rows - 1, lat_in[turn, 1][:, None, :], pltpu.roll(firsts[1], rows - 1, axis=1)),
        ]
        for which in (4, 5):
            message(turn, which).wait_recv()
        left = jnp.sum(
            jnp.where(lane == flat + flat_rows, lon_in[turn, 0], 0.0), axis=1, keepdims=True
        ).reshape(levels, rows, 1)
        right = jnp.sum(jnp.where(lane == flat, lon_in[turn, 1], 0.0), axis=1, keepdims=True).reshape(
            levels, rows, 1
        )
        below.append(jnp.where(lane3 == 0, left, pltpu.roll(lasts[2], 1, axis=2)))
        above.append(jnp.where(lane3 == cols - 1, right, pltpu.roll(firsts[2], cols - 1, axis=2)))
        return below, above

    expected = sum(1 if e is None else e.astype(jnp.int32) for _, _, e in links)
    pl.semaphore_wait(barrier, expected)
    send(0, [coarse] * 3, [coarse] * 3)

    loads[1].wait()
    numbers = courant[...].astype(jnp.float32)
    lower = [jnp.maximum(numbers[k], 0.0) for k in range(3)]
    upper = [jnp.maximum(-numbers[k], 0.0) for k in range(3)]
    centre = 1.0 - jnp.abs(numbers[0]) - jnp.abs(numbers[1]) - jnp.abs(numbers[2])

    for load in loads[2:]:
        load.wait()
    where_row = (lvl[...] - me_lev * levels) * rows + col[...] // cols
    where_col = col[...] % cols
    parts = bf16_parts(val[...], 3)
    pieces, width = col.shape
    row_id = lax.broadcasted_iota(jnp.int32, (flat_rows, width), 0)
    col_id = lax.broadcasted_iota(jnp.int32, (cols, width), 0)
    hits = [[] for _ in range(4)]
    tables = []
    for k in range(pieces):
        match = where_row[k : k + 1] == row_id
        hits[0].append(jnp.where(match, 1.0, 0.0).astype(jnp.bfloat16))
        for i, part in enumerate(parts):
            hits[i + 1].append(jnp.where(match, part[k : k + 1], 0.0).astype(jnp.bfloat16))
        tables.append(jnp.where(where_col[k : k + 1] == col_id, 1.0, 0.0).astype(jnp.bfloat16))
    left_side = jnp.concatenate([jnp.concatenate(h, axis=1) for h in hits], axis=0)
    totals = lax.dot_general(
        left_side, jnp.concatenate(tables, axis=1), (((1,), (1,)), ((), ())),
        preferred_element_type=jnp.float32,
    )
    count = totals[:flat_rows].reshape(levels, rows, cols)
    observed = (
        totals[flat_rows : 2 * flat_rows]
        + totals[2 * flat_rows : 3 * flat_rows]
        + totals[3 * flat_rows :]
    ).reshape(levels, rows, cols)

    def forward(field, turn):
        below, above = receive(turn, [field] * 3, [field] * 3)
        result = centre * field
        for k in range(3):
            result = result + lower[k] * below[k] + upper[k] * above[k]
        return result

    state = forward(coarse, 0)
    send(1, [state] * 3, [state] * 3)
    state = forward(state, 1)
    field = count * state - observed

    for turn in (2, 3):
        firsts = [lower[k] * field for k in range(3)]
        lasts = [upper[k] * field for k in range(3)]
        send(turn, firsts, lasts)
        if turn == 2:
            state_v[...] = state
        below, above = receive(turn, firsts, lasts)
        result = centre * field
        for k in range(3):
            result = result + above[k] + below[k]
        field = result
    adj_v[...] = field

    for turn in range(ROUNDS):
        for which in range(6):
            guarded(links[which][2], lambda turn=turn, which=which: message(turn, which).wait_send())


def finish(state_v, adj_v, outer, state_hbm, adj_hbm, next_hbm, wide, nxt, out_sem):
    levels, rows, cols = state_v.shape
    flat_rows = levels * rows
    wide_cols = outer.shape[1]
    fine = wide_cols // cols
    outer_rows = outer.shape[0] // levels
    stores = [
        pltpu.make_async_copy(state_v, state_hbm, out_sem.at[0]),
        pltpu.make_async_copy(adj_v, adj_hbm, out_sem.at[1]),
    ]
    for store in stores:
        store.start()
    field = adj_v[...]

    table = (
        lax.broadcasted_iota(jnp.int32, (cols, wide_cols), 0)
        == lax.broadcasted_iota(jnp.int32, (cols, wide_cols), 1) // fine
    ).astype(jnp.float32).astype(jnp.bfloat16)
    halves = bf16_parts(field.reshape(flat_rows, cols), 2)
    spread = jnp.dot(
        jnp.concatenate([h.astype(jnp.bfloat16) for h in halves], axis=1),
        jnp.concatenate([table, table], axis=0),
        preferred_element_type=jnp.float32,
    )
    for k in range(fine):
        for c in range(fine):
            wide[c, pl.ds(k, flat_rows, stride=fine), :] = spread[:, c * cols : (c + 1) * cols]
    for level in range(levels):
        span = pl.ds(level * outer_rows, outer_rows)
        for c in range(fine):
            lanes = pl.ds(c * cols, cols)
            nxt[span, lanes] = (outer[span, lanes].astype(jnp.float32) - wide[c, span, :]).astype(jnp.bfloat16)
        store = pltpu.make_async_copy(nxt.at[span], next_hbm.at[span], out_sem.at[2 + level])
        store.start()
        stores.append(store)
    for store in stores:
        store.wait()


def shards(ends, outer_increment, courant, obs_column, obs_level, obs_value):
    levels, outer_rows, wide_cols = outer_increment.shape
    _, _, rows, cols = courant.shape
    flat_rows = levels * rows
    fine = wide_cols // cols
    lanes = 128
    observed = (obs_column.shape[0] // lanes, lanes)
    assert 2 * flat_rows <= cols
    f32, bf16 = jnp.float32, jnp.bfloat16
    outer_shape = (levels * outer_rows, wide_cols)
    vmem = pl.BlockSpec(memory_space=pltpu.VMEM)
    hbm = pl.BlockSpec(memory_space=pl.ANY)
    held = pl.pallas_call(
        functools.partial(kernel, ends),
        out_shape=(
            pltpu.VMEM((levels, rows, cols), f32),
            pltpu.VMEM((levels, rows, cols), f32),
            pltpu.VMEM(outer_shape, bf16),
        ),
        in_specs=[hbm] * 5,
        out_specs=(vmem,) * 3,
        scratch_shapes=[
            pltpu.VMEM(courant.shape, bf16),
            pltpu.VMEM(observed, jnp.int32),
            pltpu.VMEM(observed, jnp.int32),
            pltpu.VMEM(observed, f32),
            pltpu.VMEM((levels * outer_rows, cols), f32),
            pltpu.VMEM((ROUNDS, 2, rows, cols), f32),
            pltpu.VMEM((ROUNDS, 2, levels, cols), f32),
            pltpu.VMEM((ROUNDS, 1, cols), f32),
            pltpu.VMEM((ROUNDS, 2, rows, cols), f32),
            pltpu.VMEM((ROUNDS, 2, levels, cols), f32),
            pltpu.VMEM((ROUNDS, 2, 1, cols), f32),
            pltpu.SemaphoreType.DMA((5,)),
            pltpu.SemaphoreType.DMA((ROUNDS, 6)),
            pltpu.SemaphoreType.DMA((ROUNDS, 6)),
        ],
        compiler_params=pltpu.CompilerParams(collective_id=0, has_side_effects=True),
    )(
        outer_increment.reshape(outer_shape),
        courant,
        obs_column.reshape(observed),
        obs_level.reshape(observed),
        obs_value.reshape(observed),
    )
    state, adjoint, following = pl.pallas_call(
        finish,
        out_shape=(
            jax.ShapeDtypeStruct((levels, rows, cols), f32),
            jax.ShapeDtypeStruct((levels, rows, cols), f32),
            jax.ShapeDtypeStruct(outer_shape, bf16),
        ),
        in_specs=[vmem] * 3,
        out_specs=(hbm,) * 3,
        scratch_shapes=[
            pltpu.VMEM((fine, levels * outer_rows, cols), f32),
            pltpu.VMEM(outer_shape, bf16),
            pltpu.SemaphoreType.DMA((2 + levels,)),
        ],
    )(*[pltpu.with_memory_space_constraint(x, pltpu.VMEM) for x in held])
    return state, adjoint, following.reshape(outer_increment.shape)


def solution(mesh):
    ends = tuple(mesh.shape[a] for a in ("lat", "lon", "lev"))
    block = P("lev", "lat", "lon")
    observed = P(("lat", "lon"))
    return jax.shard_map(
        functools.partial(shards, ends),
        mesh=mesh,
        in_specs=(block, P(None, "lev", "lat", "lon"), observed, observed, observed),
        out_specs=(block, block, block),
        check_vma=False,
    )
```

```python
import functools

import jax
import jax.numpy as jnp
from jax import lax
from jax.experimental import pallas as pl
from jax.experimental.pallas import tpu as pltpu
from jax.sharding import PartitionSpec as P

MESH = pl.DeviceIdType.MESH
ROUNDS = 3


def bf16_parts(x, count):
    parts = []
    for _ in range(count):
        part = x.astype(jnp.bfloat16).astype(jnp.float32)
        parts.append(part)
        x = x - part
    return parts


def kernel(
    ends, outer_hbm, courant_hbm, col_hbm, lvl_hbm, val_hbm,
    state_v, adj_v, outer,
    courant, col, lvl, val, sums,
    lev_out, lat_out, lon_out, lev_in, lat_in, lon_in,
    lev2_out, lat2_out, edge_out, pack_out, lev2_in, lat2_in, edge_in, pack_in,
    in_sem, send_sem, recv_sem, send2_sem, recv2_sem,
):
    n_lat, n_lon, n_lev = ends
    levels, rows, cols = state_v.shape
    flat_rows = levels * rows
    wide_cols = outer.shape[1]
    fine = wide_cols // cols

    loads = [
        pltpu.make_async_copy(src, dst, in_sem.at[i])
        for i, (src, dst) in enumerate(
            ((outer_hbm, outer), (courant_hbm, courant), (col_hbm, col), (lvl_hbm, lvl), (val_hbm, val))
        )
    ]
    for load in loads:
        load.start()

    me_lat, me_lon, me_lev = (lax.axis_index(a) for a in ("lat", "lon", "lev"))
    links = (
        ("lev", me_lev + 1, me_lev < n_lev - 1),
        ("lev", me_lev - 1, me_lev > 0),
        ("lat", me_lat + 1, me_lat < n_lat - 1),
        ("lat", me_lat - 1, me_lat > 0),
        ("lon", lax.rem(me_lon + 1, n_lon), None),
        ("lon", lax.rem(me_lon + n_lon - 1, n_lon), None),
    )
    side_lev = (links[0], links[1])
    side_lat = (links[2], links[3])
    side_lon = (links[4], links[5])

    def joined(*sides):
        exists = [e for _, _, e in sides if e is not None]
        target = {axis: who for axis, who, _ in sides}
        return target, functools.reduce(jnp.logical_and, exists) if exists else None

    wide_links = []

    def add(sides, opposite, source, landing):
        target, exists = joined(*sides)
        wide_links.append((target, exists, joined(*opposite)[1], source, landing))

    for s in range(2):
        add([side_lev[s]], [side_lev[1 - s]], lev2_out.at[s], lev2_in.at[s])
        add([side_lat[s]], [side_lat[1 - s]], lat2_out.at[s], lat2_in.at[s])
    for s in range(2):
        for t in range(2):
            add([side_lev[s], side_lat[t]], [side_lev[1 - s], side_lat[1 - t]],
                edge_out.at[2 * s + t], edge_in.at[2 * s + t])
    faces_end = len(wide_links)
    for u in range(2):
        add([side_lon[u]], [side_lon[1 - u]], pack_out, pack_in.at[u])
    for base, sides in ((2, side_lev), (6, side_lat)):
        for s in range(2):
            for u in range(2):
                add([sides[s], side_lon[u]], [sides[1 - s], side_lon[1 - u]],
                    pack_out, pack_in.at[base + 2 * s + u])
    outs = {"lev": lev_out, "lat": lat_out, "lon": lon_out}
    ins = {"lev": lev_in, "lat": lat_in, "lon": lon_in}

    def guarded(exists, action):
        if exists is None:
            action()
        else:
            pl.when(exists)(action)

    barrier = pltpu.get_barrier_semaphore()
    for target, exists, _, _, _ in wide_links:
        guarded(
            exists,
            lambda target=target: pl.semaphore_signal(
                barrier, inc=1, device_id=target, device_id_type=MESH
            ),
        )

    def wide_message(i):
        target, _, _, source, landing = wide_links[i]
        return pltpu.make_async_remote_copy(
            src_ref=source,
            dst_ref=landing,
            send_sem=send2_sem.at[i],
            recv_sem=recv2_sem.at[i],
            device_id=target,
            device_id_type=MESH,
        )

    def clear(landing):
        landing[...] = jnp.zeros(landing.shape, jnp.float32)

    for _, _, arrives, _, landing in wide_links:
        if arrives is not None:
            pl.when(jnp.logical_not(arrives))(lambda landing=landing: clear(landing))

    def message(turn, which):
        axis, who, _ = links[which]
        side = which % 2
        source = outs[axis].at[turn] if axis == "lon" else outs[axis].at[turn, side]
        return pltpu.make_async_remote_copy(
            src_ref=source,
            dst_ref=ins[axis].at[turn, side],
            send_sem=send_sem.at[turn, which],
            recv_sem=recv_sem.at[turn, which],
            device_id={axis: who},
            device_id_type=MESH,
        )

    def blank(ref, side):
        for turn in range(ROUNDS):
            ref[turn, side] = jnp.zeros(ref.shape[2:], jnp.float32)

    pl.when(me_lev == 0)(lambda: blank(lev_in, 0))
    pl.when(me_lev == n_lev - 1)(lambda: blank(lev_in, 1))
    pl.when(me_lat == 0)(lambda: blank(lat_in, 0))
    pl.when(me_lat == n_lat - 1)(lambda: blank(lat_in, 1))

    lane = lax.broadcasted_iota(jnp.int32, (flat_rows, cols), 1)
    flat = lax.broadcasted_iota(jnp.int32, (flat_rows, cols), 0)
    lane3 = lax.broadcasted_iota(jnp.int32, (levels, rows, cols), 2)
    row3 = lax.broadcasted_iota(jnp.int32, (levels, rows, cols), 1)

    pool = (
        lax.broadcasted_iota(jnp.int32, (wide_cols, cols), 0) // fine
        == lax.broadcasted_iota(jnp.int32, (wide_cols, cols), 1)
    ).astype(jnp.float32).astype(jnp.bfloat16)

    loads[0].wait()
    sums[...] = jnp.dot(outer[...], pool, preferred_element_type=jnp.float32)
    coarse = sums[pl.ds(0, flat_rows, stride=fine), :]
    for k in range(1, fine):
        coarse = coarse + sums[pl.ds(k, flat_rows, stride=fine), :]
    coarse = (coarse * (1.0 / (fine * fine))).reshape(levels, rows, cols)

    def pack(first, last):
        first = first.reshape(flat_rows, cols)[:, :1]
        last = last.reshape(flat_rows, cols)[:, cols - 1 :]
        spread = jnp.where(lane == flat, first, 0.0) + jnp.where(lane == flat + flat_rows, last, 0.0)
        return jnp.sum(spread, axis=0, keepdims=True)

    def column(row, begin, step, length):
        at = lax.broadcasted_iota(jnp.int32, (length, cols), 1)
        index = lax.broadcasted_iota(jnp.int32, (length, cols), 0)
        return jnp.sum(jnp.where(at == begin + step * index, row, 0.0), axis=1, keepdims=True)

    def either(from_previous, from_next):
        at = lax.broadcasted_iota(jnp.int32, from_next.shape, 1)
        return jnp.where(at < flat_rows, from_next, from_previous)

    def ends_of(row):
        return [column(row, b, 1, flat_rows).reshape(levels, rows, 1) for b in (flat_rows, 0)]

    def shifted(firsts, lasts, lev, lat, lon):
        below = [
            jnp.concatenate([lev[0][None], lasts[0][: levels - 1]], axis=0),
            jnp.where(row3 == 0, lat[0][:, None, :], pltpu.roll(lasts[1], 1, axis=1)),
            jnp.where(lane3 == 0, lon[0], pltpu.roll(lasts[2], 1, axis=2)),
        ]
        above = [
            jnp.concatenate([firsts[0][1:], lev[1][None]], axis=0),
            jnp.where(row3 == rows - 1, lat[1][:, None, :], pltpu.roll(firsts[1], rows - 1, axis=1)),
            jnp.where(lane3 == cols - 1, lon[1], pltpu.roll(firsts[2], cols - 1, axis=2)),
        ]
        return below, above

    def send(turn, firsts, lasts):
        lev_out[turn, 0] = lasts[0][levels - 1]
        lev_out[turn, 1] = firsts[0][0]
        lat_out[turn, 0] = lasts[1][:, rows - 1, :]
        lat_out[turn, 1] = firsts[1][:, 0, :]
        for which in range(4):
            guarded(links[which][2], lambda which=which: message(turn, which).start())
        lon_out[turn] = pack(firsts[2], lasts[2])
        for which in (4, 5):
            message(turn, which).start()

    def receive(turn):
        for which in range(6):
            guarded(links[which ^ 1][2], lambda which=which: message(turn, which).wait_recv())
        return (
            [lev_in[turn, 0], lev_in[turn, 1]],
            [lat_in[turn, 0], lat_in[turn, 1]],
            either(lon_in[turn, 0], lon_in[turn, 1]),
        )

    expected = sum(1 if link[1] is None else link[1].astype(jnp.int32) for link in wide_links)
    pl.semaphore_wait(barrier, expected)
    send(0, [coarse] * 3, [coarse] * 3)

    loads[1].wait()
    numbers = courant[...].astype(jnp.float32)
    lower = [jnp.maximum(numbers[k], 0.0) for k in range(3)]
    upper = [jnp.maximum(-numbers[k], 0.0) for k in range(3)]
    centre = 1.0 - jnp.abs(numbers[0]) - jnp.abs(numbers[1]) - jnp.abs(numbers[2])

    send(2, lower, upper)

    for load in loads[2:]:
        load.wait()
    where_row = (lvl[...] - me_lev * levels) * rows + col[...] // cols
    where_col = col[...] % cols
    parts = bf16_parts(val[...], 3)
    pieces, width = col.shape
    row_id = lax.broadcasted_iota(jnp.int32, (flat_rows, width), 0)
    col_id = lax.broadcasted_iota(jnp.int32, (cols, width), 0)
    hits = [[] for _ in range(4)]
    tables = []
    for k in range(pieces):
        match = where_row[k : k + 1] == row_id
        hits[0].append(jnp.where(match, 1.0, 0.0).astype(jnp.bfloat16))
        for i, part in enumerate(parts):
            hits[i + 1].append(jnp.where(match, part[k : k + 1], 0.0).astype(jnp.bfloat16))
        tables.append(jnp.where(where_col[k : k + 1] == col_id, 1.0, 0.0).astype(jnp.bfloat16))
    left_side = jnp.concatenate([jnp.concatenate(h, axis=1) for h in hits], axis=0)
    totals = lax.dot_general(
        left_side, jnp.concatenate(tables, axis=1), (((1,), (1,)), ((), ())),
        preferred_element_type=jnp.float32,
    )
    count = totals[:flat_rows].reshape(levels, rows, cols)
    observed = (
        totals[flat_rows : 2 * flat_rows]
        + totals[2 * flat_rows : 3 * flat_rows]
        + totals[3 * flat_rows :]
    ).reshape(levels, rows, cols)

    def forward(field, turn):
        lev, lat, lon = receive(turn)
        below, above = shifted([field] * 3, [field] * 3, lev, lat, ends_of(lon))
        result = centre * field
        for k in range(3):
            result = result + lower[k] * below[k] + upper[k] * above[k]
        return result

    state = forward(coarse, 0)
    send(1, [state] * 3, [state] * 3)
    state = forward(state, 1)
    field = count * state - observed

    state_v[...] = state
    lev3 = lax.broadcasted_iota(jnp.int32, (levels, rows, cols), 0)
    to_first = [lower[k] * field for k in range(3)]
    to_last = [upper[k] * field for k in range(3)]
    none_lev = jnp.zeros((rows, cols), jnp.float32)
    none_lat = jnp.zeros((levels, cols), jnp.float32)
    below, above = shifted(to_first, to_last, [none_lev] * 2, [none_lat] * 2, [0.0, 0.0])
    partial = centre * field
    for k in range(3):
        partial = partial + above[k] + below[k]

    last_lev, last_row = levels - 1, rows - 1
    lev_edge = (last_lev, 0)
    row_edge = (last_row, 0)
    for s in range(2):
        lev_move = (to_last, to_first)[s]
        lev2_out[s, 0] = partial[lev_edge[s]]
        lev2_out[s, 1] = lev_move[0][lev_edge[s]]
        lat2_out[s, 0] = partial[:, row_edge[s], :]
        lat2_out[s, 1] = lev_move[1][:, row_edge[s], :]
        for t in range(2):
            lat_move = (to_last, to_first)[t]
            r = row_edge[t]
            edge_out[2 * s + t, 0:1] = lat_move[1][lev_edge[s], r : r + 1, :]
            edge_out[2 * s + t, 1:2] = lev_move[0][lev_edge[s], r : r + 1, :]
    for i in range(faces_end):
        guarded(wide_links[i][1], lambda i=i: wide_message(i).start())
    moved_lon = pack(to_first[2], to_last[2])
    at_lev_ends = jnp.where(lev3 == 0, to_first[0], jnp.where(lev3 == last_lev, to_last[0], 0.0))
    at_row_ends = jnp.where(row3 == 0, to_first[1], jnp.where(row3 == last_row, to_last[1], 0.0))
    pack_out[0:1] = pack(partial, partial)
    pack_out[1:2] = moved_lon
    pack_out[2:3] = pack(at_lev_ends, at_lev_ends)
    pack_out[3:4] = pack(at_row_ends, at_row_ends)
    for i in range(faces_end, len(wide_links)):
        guarded(wide_links[i][1], lambda i=i: wide_message(i).start())

    speed_lev, speed_lat, speed_lon = receive(2)
    for i in range(len(wide_links)):
        guarded(wide_links[i][2], lambda i=i: wide_message(i).wait_recv())
    side_pack = either(pack_in[0], pack_in[1])
    lev_pack = [either(pack_in[2 + 2 * s], pack_in[3 + 2 * s]) for s in range(2)]
    lat_pack = [either(pack_in[6 + 2 * s], pack_in[7 + 2 * s]) for s in range(2)]

    left, right = ends_of(side_pack[1:2])
    field = partial + jnp.where(lane3 == 0, left, 0.0) + jnp.where(lane3 == cols - 1, right, 0.0)
    field = field + jnp.where(lev3 == 0, lev2_in[0, 1][None], 0.0)
    field = field + jnp.where(lev3 == last_lev, lev2_in[1, 1][None], 0.0)
    field = field + jnp.where(row3 == 0, lat2_in[0, 1][:, None, :], 0.0)
    field = field + jnp.where(row3 == last_row, lat2_in[1, 1][:, None, :], 0.0)

    plane_row = lax.broadcasted_iota(jnp.int32, (rows, cols), 0)
    plane_lane = lax.broadcasted_iota(jnp.int32, (rows, cols), 1)
    line_lev = lax.broadcasted_iota(jnp.int32, (levels, cols), 0)
    line_lane = lax.broadcasted_iota(jnp.int32, (levels, cols), 1)
    beside_lev, beside_lat = [], []
    for s in range(2):
        own = (to_first[0][0], to_last[0][last_lev])[s]
        plane = lev2_in[s, 0] + own
        plane = plane + jnp.where(plane_row == 0, edge_in[2 * s, 0:1], 0.0)
        plane = plane + jnp.where(plane_row == last_row, edge_in[2 * s + 1, 0:1], 0.0)
        begin = lev_edge[s] * rows
        moved = lev_pack[s][1:2]
        plane = plane + jnp.where(plane_lane == 0, column(moved, flat_rows + begin, 1, rows), 0.0)
        plane = plane + jnp.where(plane_lane == cols - 1, column(moved, begin, 1, rows), 0.0)
        beside_lev.append(plane * speed_lev[s])

        own = (to_first[1][:, 0, :], to_last[1][:, last_row, :])[s]
        plane = lat2_in[s, 0] + own
        plane = plane + jnp.where(line_lev == 0, edge_in[s, 1:2], 0.0)
        plane = plane + jnp.where(line_lev == last_lev, edge_in[2 + s, 1:2], 0.0)
        begin = row_edge[s]
        moved = lat_pack[s][1:2]
        plane = plane + jnp.where(line_lane == 0, column(moved, flat_rows + begin, rows, levels), 0.0)
        plane = plane + jnp.where(line_lane == cols - 1, column(moved, begin, rows, levels), 0.0)
        beside_lat.append(plane * speed_lat[s])
    at = lax.rem(lax.broadcasted_iota(jnp.int32, (1, cols), 1), flat_rows)
    at_lev, at_row = lax.div(at, rows), lax.rem(at, rows)
    ring = side_pack[0:1] + pltpu.roll(moved_lon, flat_rows, axis=1)
    ring = ring + jnp.where(at_lev == 0, pltpu.roll(lev_pack[0][2:3], cols - last_lev * rows, axis=1), 0.0)
    ring = ring + jnp.where(at_lev == last_lev, pltpu.roll(lev_pack[1][2:3], last_lev * rows, axis=1), 0.0)
    ring = ring + jnp.where(at_row == 0, pltpu.roll(lat_pack[0][3:4], cols - last_row, axis=1), 0.0)
    ring = ring + jnp.where(at_row == last_row, pltpu.roll(lat_pack[1][3:4], last_row, axis=1), 0.0)
    beside_lon = ends_of(ring * speed_lon)

    below, above = shifted(
        [lower[k] * field for k in range(3)], [upper[k] * field for k in range(3)],
        beside_lev, beside_lat, beside_lon,
    )
    result = centre * field
    for k in range(3):
        result = result + above[k] + below[k]
    field = result
    adj_v[...] = field

    for turn in range(ROUNDS):
        for which in range(6):
            guarded(links[which][2], lambda turn=turn, which=which: message(turn, which).wait_send())
    for i in range(len(wide_links)):
        guarded(wide_links[i][1], lambda i=i: wide_message(i).wait_send())


def finish(state_v, adj_v, outer, state_hbm, adj_hbm, next_hbm, wide, nxt, out_sem):
    levels, rows, cols = state_v.shape
    flat_rows = levels * rows
    wide_cols = outer.shape[1]
    fine = wide_cols // cols
    outer_rows = outer.shape[0] // levels
    stores = [
        pltpu.make_async_copy(state_v, state_hbm, out_sem.at[0]),
        pltpu.make_async_copy(adj_v, adj_hbm, out_sem.at[1]),
    ]
    for store in stores:
        store.start()
    field = adj_v[...]

    table = (
        lax.broadcasted_iota(jnp.int32, (cols, wide_cols), 0)
        == lax.broadcasted_iota(jnp.int32, (cols, wide_cols), 1) // fine
    ).astype(jnp.float32).astype(jnp.bfloat16)
    halves = bf16_parts(field.reshape(flat_rows, cols), 2)
    spread = jnp.dot(
        jnp.concatenate([h.astype(jnp.bfloat16) for h in halves], axis=1),
        jnp.concatenate([table, table], axis=0),
        preferred_element_type=jnp.float32,
    )
    for k in range(fine):
        for c in range(fine):
            wide[c, pl.ds(k, flat_rows, stride=fine), :] = spread[:, c * cols : (c + 1) * cols]
    for level in range(levels):
        span = pl.ds(level * outer_rows, outer_rows)
        for c in range(fine):
            lanes = pl.ds(c * cols, cols)
            nxt[span, lanes] = (outer[span, lanes].astype(jnp.float32) - wide[c, span, :]).astype(jnp.bfloat16)
        store = pltpu.make_async_copy(nxt.at[span], next_hbm.at[span], out_sem.at[2 + level])
        store.start()
        stores.append(store)
    for store in stores:
        store.wait()


def shards(ends, outer_increment, courant, obs_column, obs_level, obs_value):
    levels, outer_rows, wide_cols = outer_increment.shape
    _, _, rows, cols = courant.shape
    flat_rows = levels * rows
    fine = wide_cols // cols
    lanes = 128
    observed = (obs_column.shape[0] // lanes, lanes)
    assert 2 * flat_rows == cols and levels > 1 and rows > 1
    f32, bf16 = jnp.float32, jnp.bfloat16
    outer_shape = (levels * outer_rows, wide_cols)
    vmem = pl.BlockSpec(memory_space=pltpu.VMEM)
    hbm = pl.BlockSpec(memory_space=pl.ANY)
    held = pl.pallas_call(
        functools.partial(kernel, ends),
        out_shape=(
            pltpu.VMEM((levels, rows, cols), f32),
            pltpu.VMEM((levels, rows, cols), f32),
            pltpu.VMEM(outer_shape, bf16),
        ),
        in_specs=[hbm] * 5,
        out_specs=(vmem,) * 3,
        scratch_shapes=[
            pltpu.VMEM(courant.shape, bf16),
            pltpu.VMEM(observed, jnp.int32),
            pltpu.VMEM(observed, jnp.int32),
            pltpu.VMEM(observed, f32),
            pltpu.VMEM((levels * outer_rows, cols), f32),
            pltpu.VMEM((ROUNDS, 2, rows, cols), f32),
            pltpu.VMEM((ROUNDS, 2, levels, cols), f32),
            pltpu.VMEM((ROUNDS, 1, cols), f32),
            pltpu.VMEM((ROUNDS, 2, rows, cols), f32),
            pltpu.VMEM((ROUNDS, 2, levels, cols), f32),
            pltpu.VMEM((ROUNDS, 2, 1, cols), f32),
            pltpu.VMEM((2, 2, rows, cols), f32),
            pltpu.VMEM((2, 2, levels, cols), f32),
            pltpu.VMEM((4, 2, cols), f32),
            pltpu.VMEM((4, cols), f32),
            pltpu.VMEM((2, 2, rows, cols), f32),
            pltpu.VMEM((2, 2, levels, cols), f32),
            pltpu.VMEM((4, 2, cols), f32),
            pltpu.VMEM((10, 4, cols), f32),
            pltpu.SemaphoreType.DMA((5,)),
            pltpu.SemaphoreType.DMA((ROUNDS, 6)),
            pltpu.SemaphoreType.DMA((ROUNDS, 6)),
            pltpu.SemaphoreType.DMA((18,)),
            pltpu.SemaphoreType.DMA((18,)),
        ],
        compiler_params=pltpu.CompilerParams(collective_id=0, has_side_effects=True),
    )(
        outer_increment.reshape(outer_shape),
        courant,
        obs_column.reshape(observed),
        obs_level.reshape(observed),
        obs_value.reshape(observed),
    )
    state, adjoint, following = pl.pallas_call(
        finish,
        out_shape=(
            jax.ShapeDtypeStruct((levels, rows, cols), f32),
            jax.ShapeDtypeStruct((levels, rows, cols), f32),
            jax.ShapeDtypeStruct(outer_shape, bf16),
        ),
        in_specs=[vmem] * 3,
        out_specs=(hbm,) * 3,
        scratch_shapes=[
            pltpu.VMEM((fine, levels * outer_rows, cols), f32),
            pltpu.VMEM(outer_shape, bf16),
            pltpu.SemaphoreType.DMA((2 + levels,)),
        ],
    )(*[pltpu.with_memory_space_constraint(x, pltpu.VMEM) for x in held])
    return state, adjoint, following.reshape(outer_increment.shape)


def solution(mesh):
    ends = tuple(mesh.shape[a] for a in ("lat", "lon", "lev"))
    block = P("lev", "lat", "lon")
    observed = P(("lat", "lon"))
    return jax.shard_map(
        functools.partial(shards, ends),
        mesh=mesh,
        in_specs=(block, P(None, "lev", "lat", "lon"), observed, observed, observed),
        out_specs=(block, block, block),
        check_vma=False,
    )
```

```python
import functools

import jax
import jax.numpy as jnp
from jax import lax
from jax.experimental import pallas as pl
from jax.experimental.pallas import tpu as pltpu
from jax.sharding import PartitionSpec as P

MESH = pl.DeviceIdType.MESH
ROUNDS = 3


def bf16_parts(x, count):
    parts = []
    for _ in range(count):
        part = x.astype(jnp.bfloat16).astype(jnp.float32)
        parts.append(part)
        x = x - part
    return parts


def kernel(
    ends, outer_hbm, courant_hbm, col_hbm, lvl_hbm, val_hbm,
    state_v, adj_v, outer,
    courant, col, lvl, val, sums,
    lev_out, lat_out, lon_out, lev_in, lat_in, lon_in,
    lev2_out, lat2_out, edge_out, pack_out, lev2_in, lat2_in, edge_in, pack_in,
    in_sem, send_sem, recv_sem, send2_sem, recv2_sem,
):
    n_lat, n_lon, n_lev = ends
    levels, rows, cols = state_v.shape
    flat_rows = levels * rows
    wide_cols = outer.shape[1]
    fine = wide_cols // cols

    loads = [
        pltpu.make_async_copy(src, dst, in_sem.at[i])
        for i, (src, dst) in enumerate(
            ((outer_hbm, outer), (courant_hbm, courant), (col_hbm, col), (lvl_hbm, lvl), (val_hbm, val))
        )
    ]
    for load in loads:
        load.start()

    me_lat, me_lon, me_lev = (lax.axis_index(a) for a in ("lat", "lon", "lev"))
    links = (
        ("lev", me_lev + 1, me_lev < n_lev - 1),
        ("lev", me_lev - 1, me_lev > 0),
        ("lat", me_lat + 1, me_lat < n_lat - 1),
        ("lat", me_lat - 1, me_lat > 0),
        ("lon", lax.rem(me_lon + 1, n_lon), None),
        ("lon", lax.rem(me_lon + n_lon - 1, n_lon), None),
    )
    side_lev = (links[0], links[1])
    side_lat = (links[2], links[3])
    side_lon = (links[4], links[5])

    def joined(*sides):
        exists = [e for _, _, e in sides if e is not None]
        target = {axis: who for axis, who, _ in sides}
        return target, functools.reduce(jnp.logical_and, exists) if exists else None

    wide_links = []

    def add(sides, opposite, source, landing):
        target, exists = joined(*sides)
        wide_links.append((target, exists, joined(*opposite)[1], source, landing))

    for s in range(2):
        add([side_lev[s]], [side_lev[1 - s]], lambda q, s=s: lev2_out.at[q, s], lambda q, s=s: lev2_in.at[q, s])
        add([side_lat[s]], [side_lat[1 - s]], lambda q, s=s: lat2_out.at[q, s], lambda q, s=s: lat2_in.at[q, s])
    for s in range(2):
        for t in range(2):
            add([side_lev[s], side_lat[t]], [side_lev[1 - s], side_lat[1 - t]],
                lambda q, e=2 * s + t: edge_out.at[q, e], lambda q, e=2 * s + t: edge_in.at[q, e])
    faces_end = len(wide_links)
    for u in range(2):
        add([side_lon[u]], [side_lon[1 - u]], lambda q: pack_out.at[q], lambda q, e=u: pack_in.at[q, e])
    for base, sides in ((2, side_lev), (6, side_lat)):
        for s in range(2):
            for u in range(2):
                add([sides[s], side_lon[u]], [sides[1 - s], side_lon[1 - u]],
                    lambda q: pack_out.at[q], lambda q, e=base + 2 * s + u: pack_in.at[q, e])
    outs = {"lev": lev_out, "lat": lat_out, "lon": lon_out}
    ins = {"lev": lev_in, "lat": lat_in, "lon": lon_in}

    def guarded(exists, action):
        if exists is None:
            action()
        else:
            pl.when(exists)(action)

    barrier = pltpu.get_barrier_semaphore()
    for target, exists, _, _, _ in wide_links:
        guarded(
            exists,
            lambda target=target: pl.semaphore_signal(
                barrier, inc=1, device_id=target, device_id_type=MESH
            ),
        )

    def wide_message(q, i):
        target, _, _, source, landing = wide_links[i]
        return pltpu.make_async_remote_copy(
            src_ref=source(q),
            dst_ref=landing(q),
            send_sem=send2_sem.at[q, i],
            recv_sem=recv2_sem.at[q, i],
            device_id=target,
            device_id_type=MESH,
        )

    def clear(landing):
        for q in range(2):
            ref = landing(q)
            ref[...] = jnp.zeros(ref.shape, jnp.float32)

    for _, _, arrives, _, landing in wide_links:
        if arrives is not None:
            pl.when(jnp.logical_not(arrives))(lambda landing=landing: clear(landing))

    def message(turn, which):
        axis, who, _ = links[which]
        side = which % 2
        source = outs[axis].at[turn] if axis == "lon" else outs[axis].at[turn, side]
        return pltpu.make_async_remote_copy(
            src_ref=source,
            dst_ref=ins[axis].at[turn, side],
            send_sem=send_sem.at[turn, which],
            recv_sem=recv_sem.at[turn, which],
            device_id={axis: who},
            device_id_type=MESH,
        )

    def blank(ref, side):
        for turn in range(ROUNDS):
            ref[turn, side] = jnp.zeros(ref.shape[2:], jnp.float32)

    pl.when(me_lev == 0)(lambda: blank(lev_in, 0))
    pl.when(me_lev == n_lev - 1)(lambda: blank(lev_in, 1))
    pl.when(me_lat == 0)(lambda: blank(lat_in, 0))
    pl.when(me_lat == n_lat - 1)(lambda: blank(lat_in, 1))

    lane = lax.broadcasted_iota(jnp.int32, (flat_rows, cols), 1)
    flat = lax.broadcasted_iota(jnp.int32, (flat_rows, cols), 0)
    lane3 = lax.broadcasted_iota(jnp.int32, (levels, rows, cols), 2)
    row3 = lax.broadcasted_iota(jnp.int32, (levels, rows, cols), 1)

    pool = (
        lax.broadcasted_iota(jnp.int32, (wide_cols, cols), 0) // fine
        == lax.broadcasted_iota(jnp.int32, (wide_cols, cols), 1)
    ).astype(jnp.float32).astype(jnp.bfloat16)

    def pack(first, last):
        first = first.reshape(flat_rows, cols)[:, :1]
        last = last.reshape(flat_rows, cols)[:, cols - 1 :]
        spread = jnp.where(lane == flat, first, 0.0) + jnp.where(lane == flat + flat_rows, last, 0.0)
        return jnp.sum(spread, axis=0, keepdims=True)

    def column(row, begin, step, length):
        at = lax.broadcasted_iota(jnp.int32, (length, cols), 1)
        index = lax.broadcasted_iota(jnp.int32, (length, cols), 0)
        return jnp.sum(jnp.where(at == begin + step * index, row, 0.0), axis=1, keepdims=True)

    def either(from_previous, from_next):
        at = lax.broadcasted_iota(jnp.int32, from_next.shape, 1)
        return jnp.where(at < flat_rows, from_next, from_previous)

    def ends_of(row):
        return [column(row, b, 1, flat_rows).reshape(levels, rows, 1) for b in (flat_rows, 0)]

    def shifted(firsts, lasts, lev, lat, lon):
        below = [
            jnp.concatenate([lev[0][None], lasts[0][: levels - 1]], axis=0),
            jnp.where(row3 == 0, lat[0][:, None, :], pltpu.roll(lasts[1], 1, axis=1)),
            jnp.where(lane3 == 0, lon[0], pltpu.roll(lasts[2], 1, axis=2)),
        ]
        above = [
            jnp.concatenate([firsts[0][1:], lev[1][None]], axis=0),
            jnp.where(row3 == rows - 1, lat[1][:, None, :], pltpu.roll(firsts[1], rows - 1, axis=1)),
            jnp.where(lane3 == cols - 1, lon[1], pltpu.roll(firsts[2], cols - 1, axis=2)),
        ]
        return below, above

    def send(turn, firsts, lasts):
        lev_out[turn, 0] = lasts[0][levels - 1]
        lev_out[turn, 1] = firsts[0][0]
        lat_out[turn, 0] = lasts[1][:, rows - 1, :]
        lat_out[turn, 1] = firsts[1][:, 0, :]
        for which in range(4):
            guarded(links[which][2], lambda which=which: message(turn, which).start())
        lon_out[turn] = pack(firsts[2], lasts[2])
        for which in (4, 5):
            message(turn, which).start()

    def receive(turn):
        for which in range(6):
            guarded(links[which ^ 1][2], lambda which=which: message(turn, which).wait_recv())
        return (
            [lev_in[turn, 0], lev_in[turn, 1]],
            [lat_in[turn, 0], lat_in[turn, 1]],
            either(lon_in[turn, 0], lon_in[turn, 1]),
        )

    expected = sum(1 if link[1] is None else link[1].astype(jnp.int32) for link in wide_links)
    pl.semaphore_wait(barrier, expected)
    loads[1].wait()
    numbers = courant[...].astype(jnp.float32)
    lower = [jnp.maximum(numbers[k], 0.0) for k in range(3)]
    upper = [jnp.maximum(-numbers[k], 0.0) for k in range(3)]
    centre = 1.0 - jnp.abs(numbers[0]) - jnp.abs(numbers[1]) - jnp.abs(numbers[2])

    for k in range(3):
        send(k, [numbers[k]] * 3, [numbers[k]] * 3)

    loads[0].wait()
    sums[...] = jnp.dot(outer[...], pool, preferred_element_type=jnp.float32)
    coarse = sums[pl.ds(0, flat_rows, stride=fine), :]
    for k in range(1, fine):
        coarse = coarse + sums[pl.ds(k, flat_rows, stride=fine), :]
    coarse = (coarse * (1.0 / (fine * fine))).reshape(levels, rows, cols)

    lev3 = lax.broadcasted_iota(jnp.int32, (levels, rows, cols), 0)
    last_lev, last_row = levels - 1, rows - 1
    lev_edge = (last_lev, 0)
    row_edge = (last_row, 0)
    none_lev = jnp.zeros((rows, cols), jnp.float32)
    none_lat = jnp.zeros((levels, cols), jnp.float32)

    def step(values, lev, lat, lon):
        below, above = shifted([values] * 3, [values] * 3, lev, lat, lon)
        result = centre * values
        for k in range(3):
            result = result + lower[k] * below[k] + upper[k] * above[k]
        return result

    partial = step(coarse, [none_lev] * 2, [none_lat] * 2, [0.0, 0.0])
    for s in range(2):
        lev2_out[0, s, 0] = partial[lev_edge[s]]
        lev2_out[0, s, 1] = coarse[lev_edge[s]]
        lat2_out[0, s, 0] = partial[:, row_edge[s], :]
        lat2_out[0, s, 1] = coarse[:, row_edge[s], :]
        for t in range(2):
            for i in range(2):
                edge_out[0, 2 * s + t, i : i + 1] = coarse[lev_edge[s], row_edge[t] : row_edge[t] + 1, :]
    for i in range(faces_end):
        guarded(wide_links[i][1], lambda i=i: wide_message(0, i).start())
    own_pack = pack(coarse, coarse)
    pack_out[0, 0:1] = pack(partial, partial)
    pack_out[0, 1:2] = own_pack
    pack_out[0, 2:3] = own_pack
    pack_out[0, 3:4] = own_pack
    for i in range(faces_end, len(wide_links)):
        guarded(wide_links[i][1], lambda i=i: wide_message(0, i).start())

    for load in loads[2:]:
        load.wait()
    where_row = (lvl[...] - me_lev * levels) * rows + col[...] // cols
    where_col = col[...] % cols
    parts = bf16_parts(val[...], 3)
    pieces, width = col.shape
    row_id = lax.broadcasted_iota(jnp.int32, (flat_rows, width), 0)
    col_id = lax.broadcasted_iota(jnp.int32, (cols, width), 0)
    hits = [[] for _ in range(4)]
    tables = []
    for k in range(pieces):
        match = where_row[k : k + 1] == row_id
        hits[0].append(jnp.where(match, 1.0, 0.0).astype(jnp.bfloat16))
        for i, part in enumerate(parts):
            hits[i + 1].append(jnp.where(match, part[k : k + 1], 0.0).astype(jnp.bfloat16))
        tables.append(jnp.where(where_col[k : k + 1] == col_id, 1.0, 0.0).astype(jnp.bfloat16))
    left_side = jnp.concatenate([jnp.concatenate(h, axis=1) for h in hits], axis=0)
    totals = lax.dot_general(
        left_side, jnp.concatenate(tables, axis=1), (((1,), (1,)), ((), ())),
        preferred_element_type=jnp.float32,
    )
    count = totals[:flat_rows].reshape(levels, rows, cols)
    observed = (
        totals[flat_rows : 2 * flat_rows]
        + totals[2 * flat_rows : 3 * flat_rows]
        + totals[3 * flat_rows :]
    ).reshape(levels, rows, cols)

    plane_row = lax.broadcasted_iota(jnp.int32, (rows, cols), 0)
    plane_lane = lax.broadcasted_iota(jnp.int32, (rows, cols), 1)
    line_lev = lax.broadcasted_iota(jnp.int32, (levels, cols), 0)
    line_lane = lax.broadcasted_iota(jnp.int32, (levels, cols), 1)
    at_lane = lax.broadcasted_iota(jnp.int32, (1, cols), 1)
    at = lax.rem(at_lane, flat_rows)
    at_lev, at_row = lax.div(at, rows), lax.rem(at, rows)

    def packs(q):
        return (
            either(pack_in[q, 0], pack_in[q, 1]),
            [either(pack_in[q, 2 + 2 * s], pack_in[q, 3 + 2 * s]) for s in range(2)],
            [either(pack_in[q, 6 + 2 * s], pack_in[q, 7 + 2 * s]) for s in range(2)],
        )

    speeds = [receive(k) for k in range(3)]

    def low(x):
        return jnp.maximum(x, 0.0)

    def up(x):
        return jnp.maximum(-x, 0.0)

    for i in range(len(wide_links)):
        guarded(wide_links[i][2], lambda i=i: wide_message(0, i).wait_recv())
    side_pack, lev_pack, lat_pack = packs(0)
    beside_lev, beside_lat = [], []
    for s in range(2):
        near, far = (up, low) if s == 0 else (low, up)
        c = [speeds[k][0][s] for k in range(3)]
        plane = lev2_in[0, s, 0] + near(c[0]) * coarse[(0, last_lev)[s]]
        plane = plane + jnp.where(plane_row == 0, low(c[1]) * edge_in[0, 2 * s, 0:1], 0.0)
        plane = plane + jnp.where(plane_row == last_row, up(c[1]) * edge_in[0, 2 * s + 1, 0:1], 0.0)
        begin = lev_edge[s] * rows
        moved = lev_pack[s][1:2]
        plane = plane + jnp.where(plane_lane == 0, low(c[2]) * column(moved, flat_rows + begin, 1, rows), 0.0)
        plane = plane + jnp.where(plane_lane == cols - 1, up(c[2]) * column(moved, begin, 1, rows), 0.0)
        beside_lev.append(plane)

        c = [speeds[k][1][s] for k in range(3)]
        plane = lat2_in[0, s, 0] + near(c[1]) * coarse[:, (0, last_row)[s], :]
        plane = plane + jnp.where(line_lev == 0, low(c[0]) * edge_in[0, s, 1:2], 0.0)
        plane = plane + jnp.where(line_lev == last_lev, up(c[0]) * edge_in[0, 2 + s, 1:2], 0.0)
        begin = row_edge[s]
        moved = lat_pack[s][1:2]
        plane = plane + jnp.where(
            line_lane == 0, low(c[2]) * column(moved, flat_rows + begin, rows, levels), 0.0
        )
        plane = plane + jnp.where(line_lane == cols - 1, up(c[2]) * column(moved, begin, rows, levels), 0.0)
        beside_lat.append(plane)
    c = [speeds[k][2] for k in range(3)]
    ring = side_pack[0:1] + jnp.where(at_lane < flat_rows, low(c[2]), up(c[2])) * pltpu.roll(
        own_pack, flat_rows, axis=1
    )
    turned = [pltpu.roll(lev_pack[0][1:2], cols - last_lev * rows, axis=1), pltpu.roll(lev_pack[1][1:2], last_lev * rows, axis=1)]
    ring = ring + jnp.where(at_lev == 0, low(c[0]) * turned[0], 0.0)
    ring = ring + jnp.where(at_lev == last_lev, up(c[0]) * turned[1], 0.0)
    turned = [pltpu.roll(lat_pack[0][1:2], cols - last_row, axis=1), pltpu.roll(lat_pack[1][1:2], last_row, axis=1)]
    ring = ring + jnp.where(at_row == 0, low(c[1]) * turned[0], 0.0)
    ring = ring + jnp.where(at_row == last_row, up(c[1]) * turned[1], 0.0)

    state = step(
        coarse, [lev2_in[0, s, 1] for s in range(2)], [lat2_in[0, s, 1] for s in range(2)],
        ends_of(side_pack[1:2]),
    )
    state = step(state, beside_lev, beside_lat, ends_of(ring))
    field = count * state - observed

    state_v[...] = state
    to_first = [lower[k] * field for k in range(3)]
    to_last = [upper[k] * field for k in range(3)]
    below, above = shifted(to_first, to_last, [none_lev] * 2, [none_lat] * 2, [0.0, 0.0])
    partial = centre * field
    for k in range(3):
        partial = partial + above[k] + below[k]

    last_lev, last_row = levels - 1, rows - 1
    lev_edge = (last_lev, 0)
    row_edge = (last_row, 0)
    for s in range(2):
        lev_move = (to_last, to_first)[s]
        lev2_out[1, s, 0] = partial[lev_edge[s]]
        lev2_out[1, s, 1] = lev_move[0][lev_edge[s]]
        lat2_out[1, s, 0] = partial[:, row_edge[s], :]
        lat2_out[1, s, 1] = lev_move[1][:, row_edge[s], :]
        for t in range(2):
            lat_move = (to_last, to_first)[t]
            r = row_edge[t]
            edge_out[1, 2 * s + t, 0:1] = lat_move[1][lev_edge[s], r : r + 1, :]
            edge_out[1, 2 * s + t, 1:2] = lev_move[0][lev_edge[s], r : r + 1, :]
    for i in range(faces_end):
        guarded(wide_links[i][1], lambda i=i: wide_message(1, i).start())
    moved_lon = pack(to_first[2], to_last[2])
    at_lev_ends = jnp.where(lev3 == 0, to_first[0], jnp.where(lev3 == last_lev, to_last[0], 0.0))
    at_row_ends = jnp.where(row3 == 0, to_first[1], jnp.where(row3 == last_row, to_last[1], 0.0))
    pack_out[1, 0:1] = pack(partial, partial)
    pack_out[1, 1:2] = moved_lon
    pack_out[1, 2:3] = pack(at_lev_ends, at_lev_ends)
    pack_out[1, 3:4] = pack(at_row_ends, at_row_ends)
    for i in range(faces_end, len(wide_links)):
        guarded(wide_links[i][1], lambda i=i: wide_message(1, i).start())

    speed_lev = [up(speeds[0][0][0]), low(speeds[0][0][1])]
    speed_lat = [up(speeds[1][1][0]), low(speeds[1][1][1])]
    speed_lon = jnp.where(at_lane < flat_rows, low(speeds[2][2]), up(speeds[2][2]))
    for i in range(len(wide_links)):
        guarded(wide_links[i][2], lambda i=i: wide_message(1, i).wait_recv())
    side_pack, lev_pack, lat_pack = packs(1)

    left, right = ends_of(side_pack[1:2])
    field = partial + jnp.where(lane3 == 0, left, 0.0) + jnp.where(lane3 == cols - 1, right, 0.0)
    field = field + jnp.where(lev3 == 0, lev2_in[1, 0, 1][None], 0.0)
    field = field + jnp.where(lev3 == last_lev, lev2_in[1, 1, 1][None], 0.0)
    field = field + jnp.where(row3 == 0, lat2_in[1, 0, 1][:, None, :], 0.0)
    field = field + jnp.where(row3 == last_row, lat2_in[1, 1, 1][:, None, :], 0.0)

    plane_row = lax.broadcasted_iota(jnp.int32, (rows, cols), 0)
    plane_lane = lax.broadcasted_iota(jnp.int32, (rows, cols), 1)
    line_lev = lax.broadcasted_iota(jnp.int32, (levels, cols), 0)
    line_lane = lax.broadcasted_iota(jnp.int32, (levels, cols), 1)
    beside_lev, beside_lat = [], []
    for s in range(2):
        own = (to_first[0][0], to_last[0][last_lev])[s]
        plane = lev2_in[1, s, 0] + own
        plane = plane + jnp.where(plane_row == 0, edge_in[1, 2 * s, 0:1], 0.0)
        plane = plane + jnp.where(plane_row == last_row, edge_in[1, 2 * s + 1, 0:1], 0.0)
        begin = lev_edge[s] * rows
        moved = lev_pack[s][1:2]
        plane = plane + jnp.where(plane_lane == 0, column(moved, flat_rows + begin, 1, rows), 0.0)
        plane = plane + jnp.where(plane_lane == cols - 1, column(moved, begin, 1, rows), 0.0)
        beside_lev.append(plane * speed_lev[s])

        own = (to_first[1][:, 0, :], to_last[1][:, last_row, :])[s]
        plane = lat2_in[1, s, 0] + own
        plane = plane + jnp.where(line_lev == 0, edge_in[1, s, 1:2], 0.0)
        plane = plane + jnp.where(line_lev == last_lev, edge_in[1, 2 + s, 1:2], 0.0)
        begin = row_edge[s]
        moved = lat_pack[s][1:2]
        plane = plane + jnp.where(line_lane == 0, column(moved, flat_rows + begin, rows, levels), 0.0)
        plane = plane + jnp.where(line_lane == cols - 1, column(moved, begin, rows, levels), 0.0)
        beside_lat.append(plane * speed_lat[s])
    at = lax.rem(lax.broadcasted_iota(jnp.int32, (1, cols), 1), flat_rows)
    at_lev, at_row = lax.div(at, rows), lax.rem(at, rows)
    ring = side_pack[0:1] + pltpu.roll(moved_lon, flat_rows, axis=1)
    ring = ring + jnp.where(at_lev == 0, pltpu.roll(lev_pack[0][2:3], cols - last_lev * rows, axis=1), 0.0)
    ring = ring + jnp.where(at_lev == last_lev, pltpu.roll(lev_pack[1][2:3], last_lev * rows, axis=1), 0.0)
    ring = ring + jnp.where(at_row == 0, pltpu.roll(lat_pack[0][3:4], cols - last_row, axis=1), 0.0)
    ring = ring + jnp.where(at_row == last_row, pltpu.roll(lat_pack[1][3:4], last_row, axis=1), 0.0)
    beside_lon = ends_of(ring * speed_lon)

    below, above = shifted(
        [lower[k] * field for k in range(3)], [upper[k] * field for k in range(3)],
        beside_lev, beside_lat, beside_lon,
    )
    result = centre * field
    for k in range(3):
        result = result + above[k] + below[k]
    field = result
    adj_v[...] = field

    for turn in range(ROUNDS):
        for which in range(6):
            guarded(links[which][2], lambda turn=turn, which=which: message(turn, which).wait_send())
    for q in range(2):
        for i in range(len(wide_links)):
            guarded(wide_links[i][1], lambda q=q, i=i: wide_message(q, i).wait_send())


def finish(state_v, adj_v, outer, state_hbm, adj_hbm, next_hbm, wide, nxt, out_sem):
    levels, rows, cols = state_v.shape
    flat_rows = levels * rows
    wide_cols = outer.shape[1]
    fine = wide_cols // cols
    outer_rows = outer.shape[0] // levels
    stores = [
        pltpu.make_async_copy(state_v, state_hbm, out_sem.at[0]),
        pltpu.make_async_copy(adj_v, adj_hbm, out_sem.at[1]),
    ]
    for store in stores:
        store.start()
    field = adj_v[...]

    table = (
        lax.broadcasted_iota(jnp.int32, (cols, wide_cols), 0)
        == lax.broadcasted_iota(jnp.int32, (cols, wide_cols), 1) // fine
    ).astype(jnp.float32).astype(jnp.bfloat16)
    halves = bf16_parts(field.reshape(flat_rows, cols), 2)
    spread = jnp.dot(
        jnp.concatenate([h.astype(jnp.bfloat16) for h in halves], axis=1),
        jnp.concatenate([table, table], axis=0),
        preferred_element_type=jnp.float32,
    )
    for k in range(fine):
        for c in range(fine):
            wide[c, pl.ds(k, flat_rows, stride=fine), :] = spread[:, c * cols : (c + 1) * cols]
    for level in range(levels):
        span = pl.ds(level * outer_rows, outer_rows)
        for c in range(fine):
            lanes = pl.ds(c * cols, cols)
            nxt[span, lanes] = (outer[span, lanes].astype(jnp.float32) - wide[c, span, :]).astype(jnp.bfloat16)
        store = pltpu.make_async_copy(nxt.at[span], next_hbm.at[span], out_sem.at[2 + level])
        store.start()
        stores.append(store)
    for store in stores:
        store.wait()


def shards(ends, outer_increment, courant, obs_column, obs_level, obs_value):
    levels, outer_rows, wide_cols = outer_increment.shape
    _, _, rows, cols = courant.shape
    flat_rows = levels * rows
    fine = wide_cols // cols
    lanes = 128
    observed = (obs_column.shape[0] // lanes, lanes)
    assert 2 * flat_rows == cols and levels > 1 and rows > 1
    f32, bf16 = jnp.float32, jnp.bfloat16
    outer_shape = (levels * outer_rows, wide_cols)
    vmem = pl.BlockSpec(memory_space=pltpu.VMEM)
    hbm = pl.BlockSpec(memory_space=pl.ANY)
    held = pl.pallas_call(
        functools.partial(kernel, ends),
        out_shape=(
            pltpu.VMEM((levels, rows, cols), f32),
            pltpu.VMEM((levels, rows, cols), f32),
            pltpu.VMEM(outer_shape, bf16),
        ),
        in_specs=[hbm] * 5,
        out_specs=(vmem,) * 3,
        scratch_shapes=[
            pltpu.VMEM(courant.shape, bf16),
            pltpu.VMEM(observed, jnp.int32),
            pltpu.VMEM(observed, jnp.int32),
            pltpu.VMEM(observed, f32),
            pltpu.VMEM((levels * outer_rows, cols), f32),
            pltpu.VMEM((ROUNDS, 2, rows, cols), f32),
            pltpu.VMEM((ROUNDS, 2, levels, cols), f32),
            pltpu.VMEM((ROUNDS, 1, cols), f32),
            pltpu.VMEM((ROUNDS, 2, rows, cols), f32),
            pltpu.VMEM((ROUNDS, 2, levels, cols), f32),
            pltpu.VMEM((ROUNDS, 2, 1, cols), f32),
            pltpu.VMEM((2, 2, 2, rows, cols), f32),
            pltpu.VMEM((2, 2, 2, levels, cols), f32),
            pltpu.VMEM((2, 4, 2, cols), f32),
            pltpu.VMEM((2, 4, cols), f32),
            pltpu.VMEM((2, 2, 2, rows, cols), f32),
            pltpu.VMEM((2, 2, 2, levels, cols), f32),
            pltpu.VMEM((2, 4, 2, cols), f32),
            pltpu.VMEM((2, 10, 4, cols), f32),
            pltpu.SemaphoreType.DMA((5,)),
            pltpu.SemaphoreType.DMA((ROUNDS, 6)),
            pltpu.SemaphoreType.DMA((ROUNDS, 6)),
            pltpu.SemaphoreType.DMA((2, 18)),
            pltpu.SemaphoreType.DMA((2, 18)),
        ],
        compiler_params=pltpu.CompilerParams(collective_id=0, has_side_effects=True),
    )(
        outer_increment.reshape(outer_shape),
        courant,
        obs_column.reshape(observed),
        obs_level.reshape(observed),
        obs_value.reshape(observed),
    )
    state, adjoint, following = pl.pallas_call(
        finish,
        out_shape=(
            jax.ShapeDtypeStruct((levels, rows, cols), f32),
            jax.ShapeDtypeStruct((levels, rows, cols), f32),
            jax.ShapeDtypeStruct(outer_shape, bf16),
        ),
        in_specs=[vmem] * 3,
        out_specs=(hbm,) * 3,
        scratch_shapes=[
            pltpu.VMEM((fine, levels * outer_rows, cols), f32),
            pltpu.VMEM(outer_shape, bf16),
            pltpu.SemaphoreType.DMA((2 + levels,)),
        ],
    )(*[pltpu.with_memory_space_constraint(x, pltpu.VMEM) for x in held])
    return state, adjoint, following.reshape(outer_increment.shape)


def solution(mesh):
    ends = tuple(mesh.shape[a] for a in ("lat", "lon", "lev"))
    block = P("lev", "lat", "lon")
    observed = P(("lat", "lon"))
    return jax.shard_map(
        functools.partial(shards, ends),
        mesh=mesh,
        in_specs=(block, P(None, "lev", "lat", "lon"), observed, observed, observed),
        out_specs=(block, block, block),
        check_vma=False,
    )
```

```python
import functools

import jax
import jax.numpy as jnp
from jax import lax
from jax.experimental import pallas as pl
from jax.experimental.pallas import tpu as pltpu
from jax.sharding import PartitionSpec as P

MESH = pl.DeviceIdType.MESH
ROUNDS = 3


def bf16_parts(x, count):
    parts = []
    for _ in range(count):
        part = x.astype(jnp.bfloat16).astype(jnp.float32)
        parts.append(part)
        x = x - part
    return parts


def kernel(
    ends, outer_hbm, courant_hbm, col_hbm, lvl_hbm, val_hbm,
    state_v, adj_v, outer,
    courant, col, lvl, val, sums,
    lev_out, lat_out, lon_out, lev_in, lat_in, lon_in,
    lev2_out, lat2_out, edge_out, pack_out, lev2_in, lat2_in, edge_in, pack_in,
    in_sem, send_sem, recv_sem, send2_sem, recv2_sem,
):
    n_lat, n_lon, n_lev = ends
    levels, rows, cols = state_v.shape
    flat_rows = levels * rows
    wide_cols = outer.shape[1]
    fine = wide_cols // cols

    loads = [
        pltpu.make_async_copy(src, dst, in_sem.at[i])
        for i, (src, dst) in enumerate(
            ((outer_hbm, outer), (courant_hbm, courant), (col_hbm, col), (lvl_hbm, lvl), (val_hbm, val))
        )
    ]
    for load in loads:
        load.start()

    me_lat, me_lon, me_lev = (lax.axis_index(a) for a in ("lat", "lon", "lev"))
    links = (
        ("lev", me_lev + 1, me_lev < n_lev - 1),
        ("lev", me_lev - 1, me_lev > 0),
        ("lat", me_lat + 1, me_lat < n_lat - 1),
        ("lat", me_lat - 1, me_lat > 0),
        ("lon", lax.rem(me_lon + 1, n_lon), None),
        ("lon", lax.rem(me_lon + n_lon - 1, n_lon), None),
    )
    side_lev = (links[0], links[1])
    side_lat = (links[2], links[3])
    side_lon = (links[4], links[5])

    def joined(*sides):
        exists = [e for _, _, e in sides if e is not None]
        target = {axis: who for axis, who, _ in sides}
        return target, functools.reduce(jnp.logical_and, exists) if exists else None

    wide_links = []

    def add(sides, opposite, source, landing):
        target, exists = joined(*sides)
        wide_links.append((target, exists, joined(*opposite)[1], source, landing))

    for s in range(2):
        add([side_lev[s]], [side_lev[1 - s]], lambda q, s=s: lev2_out.at[q, s], lambda q, s=s: lev2_in.at[q, s])
        add([side_lat[s]], [side_lat[1 - s]], lambda q, s=s: lat2_out.at[q, s], lambda q, s=s: lat2_in.at[q, s])
    for s in range(2):
        for t in range(2):
            add([side_lev[s], side_lat[t]], [side_lev[1 - s], side_lat[1 - t]],
                lambda q, e=2 * s + t: edge_out.at[q, e], lambda q, e=2 * s + t: edge_in.at[q, e])
    faces_end = len(wide_links)
    for u in range(2):
        add([side_lon[u]], [side_lon[1 - u]], lambda q: pack_out.at[q], lambda q, e=u: pack_in.at[q, e])
    for base, sides in ((2, side_lev), (6, side_lat)):
        for s in range(2):
            for u in range(2):
                add([sides[s], side_lon[u]], [sides[1 - s], side_lon[1 - u]],
                    lambda q: pack_out.at[q], lambda q, e=base + 2 * s + u: pack_in.at[q, e])
    outs = {"lev": lev_out, "lat": lat_out, "lon": lon_out}
    ins = {"lev": lev_in, "lat": lat_in, "lon": lon_in}

    def guarded(exists, action):
        if exists is None:
            action()
        else:
            pl.when(exists)(action)

    barrier = pltpu.get_barrier_semaphore()
    for target, exists, _, _, _ in wide_links:
        guarded(
            exists,
            lambda target=target: pl.semaphore_signal(
                barrier, inc=1, device_id=target, device_id_type=MESH
            ),
        )

    def wide_message(q, i):
        target, _, _, source, landing = wide_links[i]
        return pltpu.make_async_remote_copy(
            src_ref=source(q),
            dst_ref=landing(q),
            send_sem=send2_sem.at[q, i],
            recv_sem=recv2_sem.at[q, i],
            device_id=target,
            device_id_type=MESH,
        )

    def clear(landing):
        for q in range(2):
            ref = landing(q)
            ref[...] = jnp.zeros(ref.shape, jnp.float32)

    for _, _, arrives, _, landing in wide_links:
        if arrives is not None:
            pl.when(jnp.logical_not(arrives))(lambda landing=landing: clear(landing))

    def message(turn, which):
        axis, who, _ = links[which]
        side = which % 2
        source = outs[axis].at[turn] if axis == "lon" else outs[axis].at[turn, side]
        return pltpu.make_async_remote_copy(
            src_ref=source,
            dst_ref=ins[axis].at[turn, side],
            send_sem=send_sem.at[turn, which],
            recv_sem=recv_sem.at[turn, which],
            device_id={axis: who},
            device_id_type=MESH,
        )

    def blank(ref, side):
        for turn in range(ROUNDS):
            ref[turn, side] = jnp.zeros(ref.shape[2:], jnp.float32)

    pl.when(me_lev == 0)(lambda: blank(lev_in, 0))
    pl.when(me_lev == n_lev - 1)(lambda: blank(lev_in, 1))
    pl.when(me_lat == 0)(lambda: blank(lat_in, 0))
    pl.when(me_lat == n_lat - 1)(lambda: blank(lat_in, 1))

    lane = lax.broadcasted_iota(jnp.int32, (flat_rows, cols), 1)
    flat = lax.broadcasted_iota(jnp.int32, (flat_rows, cols), 0)
    lane3 = lax.broadcasted_iota(jnp.int32, (levels, rows, cols), 2)
    row3 = lax.broadcasted_iota(jnp.int32, (levels, rows, cols), 1)

    pool = (
        lax.broadcasted_iota(jnp.int32, (wide_cols, cols), 0) // fine
        == lax.broadcasted_iota(jnp.int32, (wide_cols, cols), 1)
    ).astype(jnp.float32).astype(jnp.bfloat16)

    def pack(first, last):
        first = first.reshape(flat_rows, cols)[:, :1]
        last = last.reshape(flat_rows, cols)[:, cols - 1 :]
        spread = jnp.where(lane == flat, first, 0.0) + jnp.where(lane == flat + flat_rows, last, 0.0)
        return jnp.sum(spread, axis=0, keepdims=True)

    def column(row, begin, step, length):
        at = lax.broadcasted_iota(jnp.int32, (length, cols), 1)
        index = lax.broadcasted_iota(jnp.int32, (length, cols), 0)
        return jnp.sum(jnp.where(at == begin + step * index, row, 0.0), axis=1, keepdims=True)

    def either(from_previous, from_next):
        at = lax.broadcasted_iota(jnp.int32, from_next.shape, 1)
        return jnp.where(at < flat_rows, from_next, from_previous)

    def ends_of(row):
        return [column(row, b, 1, flat_rows).reshape(levels, rows, 1) for b in (flat_rows, 0)]

    def shifted(firsts, lasts, lev, lat, lon):
        below = [
            jnp.concatenate([lev[0][None], lasts[0][: levels - 1]], axis=0),
            jnp.where(row3 == 0, lat[0][:, None, :], pltpu.roll(lasts[1], 1, axis=1)),
            jnp.where(lane3 == 0, lon[0], pltpu.roll(lasts[2], 1, axis=2)),
        ]
        above = [
            jnp.concatenate([firsts[0][1:], lev[1][None]], axis=0),
            jnp.where(row3 == rows - 1, lat[1][:, None, :], pltpu.roll(firsts[1], rows - 1, axis=1)),
            jnp.where(lane3 == cols - 1, lon[1], pltpu.roll(firsts[2], cols - 1, axis=2)),
        ]
        return below, above

    def send(turn, firsts, lasts):
        lev_out[turn, 0] = lasts[0][levels - 1]
        lev_out[turn, 1] = firsts[0][0]
        lat_out[turn, 0] = lasts[1][:, rows - 1, :]
        lat_out[turn, 1] = firsts[1][:, 0, :]
        for which in range(4):
            guarded(links[which][2], lambda which=which: message(turn, which).start())
        lon_out[turn] = pack(firsts[2], lasts[2])
        for which in (4, 5):
            message(turn, which).start()

    def receive(turn):
        for which in range(6):
            guarded(links[which ^ 1][2], lambda which=which: message(turn, which).wait_recv())
        return (
            [lev_in[turn, 0], lev_in[turn, 1]],
            [lat_in[turn, 0], lat_in[turn, 1]],
            either(lon_in[turn, 0], lon_in[turn, 1]),
        )

    expected = sum(1 if link[1] is None else link[1].astype(jnp.int32) for link in wide_links)
    loads[1].wait()
    numbers = courant[...].astype(jnp.float32)
    lower = [jnp.maximum(numbers[k], 0.0) for k in range(3)]
    upper = [jnp.maximum(-numbers[k], 0.0) for k in range(3)]
    centre = 1.0 - jnp.abs(numbers[0]) - jnp.abs(numbers[1]) - jnp.abs(numbers[2])

    loads[0].wait()
    sums[...] = jnp.dot(outer[...], pool, preferred_element_type=jnp.float32)
    coarse = sums[pl.ds(0, flat_rows, stride=fine), :]
    for k in range(1, fine):
        coarse = coarse + sums[pl.ds(k, flat_rows, stride=fine), :]
    coarse = (coarse * (1.0 / (fine * fine))).reshape(levels, rows, cols)

    lev3 = lax.broadcasted_iota(jnp.int32, (levels, rows, cols), 0)
    last_lev, last_row = levels - 1, rows - 1
    lev_edge = (last_lev, 0)
    row_edge = (last_row, 0)
    none_lev = jnp.zeros((rows, cols), jnp.float32)
    none_lat = jnp.zeros((levels, cols), jnp.float32)

    def step(values, lev, lat, lon):
        below, above = shifted([values] * 3, [values] * 3, lev, lat, lon)
        result = centre * values
        for k in range(3):
            result = result + lower[k] * below[k] + upper[k] * above[k]
        return result

    partial = step(coarse, [none_lev] * 2, [none_lat] * 2, [0.0, 0.0])
    pl.semaphore_wait(barrier, expected)
    for s in range(2):
        lev2_out[0, s, 0] = partial[lev_edge[s]]
        lev2_out[0, s, 1] = coarse[lev_edge[s]]
        lat2_out[0, s, 0] = partial[:, row_edge[s], :]
        lat2_out[0, s, 1] = coarse[:, row_edge[s], :]
        for t in range(2):
            for i in range(2):
                edge_out[0, 2 * s + t, i : i + 1] = coarse[lev_edge[s], row_edge[t] : row_edge[t] + 1, :]
    for i in range(faces_end):
        guarded(wide_links[i][1], lambda i=i: wide_message(0, i).start())
    own_pack = pack(coarse, coarse)
    pack_out[0, 0:1] = pack(partial, partial)
    pack_out[0, 1:2] = own_pack
    pack_out[0, 2:3] = own_pack
    pack_out[0, 3:4] = own_pack
    for i in range(faces_end, len(wide_links)):
        guarded(wide_links[i][1], lambda i=i: wide_message(0, i).start())

    for k in range(3):
        send(k, [numbers[k]] * 3, [numbers[k]] * 3)

    for load in loads[2:]:
        load.wait()
    where_row = (lvl[...] - me_lev * levels) * rows + col[...] // cols
    where_col = col[...] % cols
    parts = bf16_parts(val[...], 3)
    pieces, width = col.shape
    row_id = lax.broadcasted_iota(jnp.int32, (flat_rows, width), 0)
    col_id = lax.broadcasted_iota(jnp.int32, (cols, width), 0)
    hits = [[] for _ in range(4)]
    tables = []
    for k in range(pieces):
        match = where_row[k : k + 1] == row_id
        hits[0].append(jnp.where(match, 1.0, 0.0).astype(jnp.bfloat16))
        for i, part in enumerate(parts):
            hits[i + 1].append(jnp.where(match, part[k : k + 1], 0.0).astype(jnp.bfloat16))
        tables.append(jnp.where(where_col[k : k + 1] == col_id, 1.0, 0.0).astype(jnp.bfloat16))
    left_side = jnp.concatenate([jnp.concatenate(h, axis=1) for h in hits], axis=0)
    totals = lax.dot_general(
        left_side, jnp.concatenate(tables, axis=1), (((1,), (1,)), ((), ())),
        preferred_element_type=jnp.float32,
    )
    count = totals[:flat_rows].reshape(levels, rows, cols)
    observed = (
        totals[flat_rows : 2 * flat_rows]
        + totals[2 * flat_rows : 3 * flat_rows]
        + totals[3 * flat_rows :]
    ).reshape(levels, rows, cols)

    plane_row = lax.broadcasted_iota(jnp.int32, (rows, cols), 0)
    plane_lane = lax.broadcasted_iota(jnp.int32, (rows, cols), 1)
    line_lev = lax.broadcasted_iota(jnp.int32, (levels, cols), 0)
    line_lane = lax.broadcasted_iota(jnp.int32, (levels, cols), 1)
    at_lane = lax.broadcasted_iota(jnp.int32, (1, cols), 1)
    at = lax.rem(at_lane, flat_rows)
    at_lev, at_row = lax.div(at, rows), lax.rem(at, rows)

    def packs(q):
        return (
            either(pack_in[q, 0], pack_in[q, 1]),
            [either(pack_in[q, 2 + 2 * s], pack_in[q, 3 + 2 * s]) for s in range(2)],
            [either(pack_in[q, 6 + 2 * s], pack_in[q, 7 + 2 * s]) for s in range(2)],
        )

    speeds = [receive(k) for k in range(3)]

    def low(x):
        return jnp.maximum(x, 0.0)

    def up(x):
        return jnp.maximum(-x, 0.0)

    for i in range(len(wide_links)):
        guarded(wide_links[i][2], lambda i=i: wide_message(0, i).wait_recv())
    side_pack, lev_pack, lat_pack = packs(0)
    beside_lev, beside_lat = [], []
    for s in range(2):
        near, far = (up, low) if s == 0 else (low, up)
        c = [speeds[k][0][s] for k in range(3)]
        plane = lev2_in[0, s, 0] + near(c[0]) * coarse[(0, last_lev)[s]]
        plane = plane + jnp.where(plane_row == 0, low(c[1]) * edge_in[0, 2 * s, 0:1], 0.0)
        plane = plane + jnp.where(plane_row == last_row, up(c[1]) * edge_in[0, 2 * s + 1, 0:1], 0.0)
        begin = lev_edge[s] * rows
        moved = lev_pack[s][1:2]
        plane = plane + jnp.where(plane_lane == 0, low(c[2]) * column(moved, flat_rows + begin, 1, rows), 0.0)
        plane = plane + jnp.where(plane_lane == cols - 1, up(c[2]) * column(moved, begin, 1, rows), 0.0)
        beside_lev.append(plane)

        c = [speeds[k][1][s] for k in range(3)]
        plane = lat2_in[0, s, 0] + near(c[1]) * coarse[:, (0, last_row)[s], :]
        plane = plane + jnp.where(line_lev == 0, low(c[0]) * edge_in[0, s, 1:2], 0.0)
        plane = plane + jnp.where(line_lev == last_lev, up(c[0]) * edge_in[0, 2 + s, 1:2], 0.0)
        begin = row_edge[s]
        moved = lat_pack[s][1:2]
        plane = plane + jnp.where(
            line_lane == 0, low(c[2]) * column(moved, flat_rows + begin, rows, levels), 0.0
        )
        plane = plane + jnp.where(line_lane == cols - 1, up(c[2]) * column(moved, begin, rows, levels), 0.0)
        beside_lat.append(plane)
    c = [speeds[k][2] for k in range(3)]
    ring = side_pack[0:1] + jnp.where(at_lane < flat_rows, low(c[2]), up(c[2])) * pltpu.roll(
        own_pack, flat_rows, axis=1
    )
    turned = [pltpu.roll(lev_pack[0][1:2], cols - last_lev * rows, axis=1), pltpu.roll(lev_pack[1][1:2], last_lev * rows, axis=1)]
    ring = ring + jnp.where(at_lev == 0, low(c[0]) * turned[0], 0.0)
    ring = ring + jnp.where(at_lev == last_lev, up(c[0]) * turned[1], 0.0)
    turned = [pltpu.roll(lat_pack[0][1:2], cols - last_row, axis=1), pltpu.roll(lat_pack[1][1:2], last_row, axis=1)]
    ring = ring + jnp.where(at_row == 0, low(c[1]) * turned[0], 0.0)
    ring = ring + jnp.where(at_row == last_row, up(c[1]) * turned[1], 0.0)

    state = step(
        coarse, [lev2_in[0, s, 1] for s in range(2)], [lat2_in[0, s, 1] for s in range(2)],
        ends_of(side_pack[1:2]),
    )
    state = step(state, beside_lev, beside_lat, ends_of(ring))
    field = count * state - observed

    state_v[...] = state
    to_first = [lower[k] * field for k in range(3)]
    to_last = [upper[k] * field for k in range(3)]
    below, above = shifted(to_first, to_last, [none_lev] * 2, [none_lat] * 2, [0.0, 0.0])
    partial = centre * field
    for k in range(3):
        partial = partial + above[k] + below[k]

    last_lev, last_row = levels - 1, rows - 1
    lev_edge = (last_lev, 0)
    row_edge = (last_row, 0)
    for s in range(2):
        lev_move = (to_last, to_first)[s]
        lev2_out[1, s, 0] = partial[lev_edge[s]]
        lev2_out[1, s, 1] = lev_move[0][lev_edge[s]]
        lat2_out[1, s, 0] = partial[:, row_edge[s], :]
        lat2_out[1, s, 1] = lev_move[1][:, row_edge[s], :]
        for t in range(2):
            lat_move = (to_last, to_first)[t]
            r = row_edge[t]
            edge_out[1, 2 * s + t, 0:1] = lat_move[1][lev_edge[s], r : r + 1, :]
            edge_out[1, 2 * s + t, 1:2] = lev_move[0][lev_edge[s], r : r + 1, :]
    for i in range(faces_end):
        guarded(wide_links[i][1], lambda i=i: wide_message(1, i).start())
    moved_lon = pack(to_first[2], to_last[2])
    at_lev_ends = jnp.where(lev3 == 0, to_first[0], jnp.where(lev3 == last_lev, to_last[0], 0.0))
    at_row_ends = jnp.where(row3 == 0, to_first[1], jnp.where(row3 == last_row, to_last[1], 0.0))
    pack_out[1, 0:1] = pack(partial, partial)
    pack_out[1, 1:2] = moved_lon
    pack_out[1, 2:3] = pack(at_lev_ends, at_lev_ends)
    pack_out[1, 3:4] = pack(at_row_ends, at_row_ends)
    for i in range(faces_end, len(wide_links)):
        guarded(wide_links[i][1], lambda i=i: wide_message(1, i).start())

    speed_lev = [up(speeds[0][0][0]), low(speeds[0][0][1])]
    speed_lat = [up(speeds[1][1][0]), low(speeds[1][1][1])]
    speed_lon = jnp.where(at_lane < flat_rows, low(speeds[2][2]), up(speeds[2][2]))
    for i in range(len(wide_links)):
        guarded(wide_links[i][2], lambda i=i: wide_message(1, i).wait_recv())
    side_pack, lev_pack, lat_pack = packs(1)

    left, right = ends_of(side_pack[1:2])
    field = partial + jnp.where(lane3 == 0, left, 0.0) + jnp.where(lane3 == cols - 1, right, 0.0)
    field = field + jnp.where(lev3 == 0, lev2_in[1, 0, 1][None], 0.0)
    field = field + jnp.where(lev3 == last_lev, lev2_in[1, 1, 1][None], 0.0)
    field = field + jnp.where(row3 == 0, lat2_in[1, 0, 1][:, None, :], 0.0)
    field = field + jnp.where(row3 == last_row, lat2_in[1, 1, 1][:, None, :], 0.0)

    plane_row = lax.broadcasted_iota(jnp.int32, (rows, cols), 0)
    plane_lane = lax.broadcasted_iota(jnp.int32, (rows, cols), 1)
    line_lev = lax.broadcasted_iota(jnp.int32, (levels, cols), 0)
    line_lane = lax.broadcasted_iota(jnp.int32, (levels, cols), 1)
    beside_lev, beside_lat = [], []
    for s in range(2):
        own = (to_first[0][0], to_last[0][last_lev])[s]
        plane = lev2_in[1, s, 0] + own
        plane = plane + jnp.where(plane_row == 0, edge_in[1, 2 * s, 0:1], 0.0)
        plane = plane + jnp.where(plane_row == last_row, edge_in[1, 2 * s + 1, 0:1], 0.0)
        begin = lev_edge[s] * rows
        moved = lev_pack[s][1:2]
        plane = plane + jnp.where(plane_lane == 0, column(moved, flat_rows + begin, 1, rows), 0.0)
        plane = plane + jnp.where(plane_lane == cols - 1, column(moved, begin, 1, rows), 0.0)
        beside_lev.append(plane * speed_lev[s])

        own = (to_first[1][:, 0, :], to_last[1][:, last_row, :])[s]
        plane = lat2_in[1, s, 0] + own
        plane = plane + jnp.where(line_lev == 0, edge_in[1, s, 1:2], 0.0)
        plane = plane + jnp.where(line_lev == last_lev, edge_in[1, 2 + s, 1:2], 0.0)
        begin = row_edge[s]
        moved = lat_pack[s][1:2]
        plane = plane + jnp.where(line_lane == 0, column(moved, flat_rows + begin, rows, levels), 0.0)
        plane = plane + jnp.where(line_lane == cols - 1, column(moved, begin, rows, levels), 0.0)
        beside_lat.append(plane * speed_lat[s])
    at = lax.rem(lax.broadcasted_iota(jnp.int32, (1, cols), 1), flat_rows)
    at_lev, at_row = lax.div(at, rows), lax.rem(at, rows)
    ring = side_pack[0:1] + pltpu.roll(moved_lon, flat_rows, axis=1)
    ring = ring + jnp.where(at_lev == 0, pltpu.roll(lev_pack[0][2:3], cols - last_lev * rows, axis=1), 0.0)
    ring = ring + jnp.where(at_lev == last_lev, pltpu.roll(lev_pack[1][2:3], last_lev * rows, axis=1), 0.0)
    ring = ring + jnp.where(at_row == 0, pltpu.roll(lat_pack[0][3:4], cols - last_row, axis=1), 0.0)
    ring = ring + jnp.where(at_row == last_row, pltpu.roll(lat_pack[1][3:4], last_row, axis=1), 0.0)
    beside_lon = ends_of(ring * speed_lon)

    below, above = shifted(
        [lower[k] * field for k in range(3)], [upper[k] * field for k in range(3)],
        beside_lev, beside_lat, beside_lon,
    )
    result = centre * field
    for k in range(3):
        result = result + above[k] + below[k]
    field = result
    adj_v[...] = field

    for turn in range(ROUNDS):
        for which in range(6):
            guarded(links[which][2], lambda turn=turn, which=which: message(turn, which).wait_send())
    for q in range(2):
        for i in range(len(wide_links)):
            guarded(wide_links[i][1], lambda q=q, i=i: wide_message(q, i).wait_send())


def finish(state_v, adj_v, outer, state_hbm, adj_hbm, next_hbm, wide, nxt, out_sem):
    levels, rows, cols = state_v.shape
    flat_rows = levels * rows
    wide_cols = outer.shape[1]
    fine = wide_cols // cols
    outer_rows = outer.shape[0] // levels
    stores = [
        pltpu.make_async_copy(state_v, state_hbm, out_sem.at[0]),
        pltpu.make_async_copy(adj_v, adj_hbm, out_sem.at[1]),
    ]
    for store in stores:
        store.start()
    field = adj_v[...]

    table = (
        lax.broadcasted_iota(jnp.int32, (cols, wide_cols), 0)
        == lax.broadcasted_iota(jnp.int32, (cols, wide_cols), 1) // fine
    ).astype(jnp.float32).astype(jnp.bfloat16)
    halves = bf16_parts(field.reshape(flat_rows, cols), 2)
    spread = jnp.dot(
        jnp.concatenate([h.astype(jnp.bfloat16) for h in halves], axis=1),
        jnp.concatenate([table, table], axis=0),
        preferred_element_type=jnp.float32,
    )
    for k in range(fine):
        for c in range(fine):
            wide[c, pl.ds(k, flat_rows, stride=fine), :] = spread[:, c * cols : (c + 1) * cols]
    for level in range(levels):
        span = pl.ds(level * outer_rows, outer_rows)
        for c in range(fine):
            lanes = pl.ds(c * cols, cols)
            nxt[span, lanes] = (outer[span, lanes].astype(jnp.float32) - wide[c, span, :]).astype(jnp.bfloat16)
        store = pltpu.make_async_copy(nxt.at[span], next_hbm.at[span], out_sem.at[2 + level])
        store.start()
        stores.append(store)
    for store in stores:
        store.wait()


def shards(ends, outer_increment, courant, obs_column, obs_level, obs_value):
    levels, outer_rows, wide_cols = outer_increment.shape
    _, _, rows, cols = courant.shape
    flat_rows = levels * rows
    fine = wide_cols // cols
    lanes = 128
    observed = (obs_column.shape[0] // lanes, lanes)
    assert 2 * flat_rows == cols and levels > 1 and rows > 1
    f32, bf16 = jnp.float32, jnp.bfloat16
    outer_shape = (levels * outer_rows, wide_cols)
    vmem = pl.BlockSpec(memory_space=pltpu.VMEM)
    hbm = pl.BlockSpec(memory_space=pl.ANY)
    held = pl.pallas_call(
        functools.partial(kernel, ends),
        out_shape=(
            pltpu.VMEM((levels, rows, cols), f32),
            pltpu.VMEM((levels, rows, cols), f32),
            pltpu.VMEM(outer_shape, bf16),
        ),
        in_specs=[hbm] * 5,
        out_specs=(vmem,) * 3,
        scratch_shapes=[
            pltpu.VMEM(courant.shape, bf16),
            pltpu.VMEM(observed, jnp.int32),
            pltpu.VMEM(observed, jnp.int32),
            pltpu.VMEM(observed, f32),
            pltpu.VMEM((levels * outer_rows, cols), f32),
            pltpu.VMEM((ROUNDS, 2, rows, cols), f32),
            pltpu.VMEM((ROUNDS, 2, levels, cols), f32),
            pltpu.VMEM((ROUNDS, 1, cols), f32),
            pltpu.VMEM((ROUNDS, 2, rows, cols), f32),
            pltpu.VMEM((ROUNDS, 2, levels, cols), f32),
            pltpu.VMEM((ROUNDS, 2, 1, cols), f32),
            pltpu.VMEM((2, 2, 2, rows, cols), f32),
            pltpu.VMEM((2, 2, 2, levels, cols), f32),
            pltpu.VMEM((2, 4, 2, cols), f32),
            pltpu.VMEM((2, 4, cols), f32),
            pltpu.VMEM((2, 2, 2, rows, cols), f32),
            pltpu.VMEM((2, 2, 2, levels, cols), f32),
            pltpu.VMEM((2, 4, 2, cols), f32),
            pltpu.VMEM((2, 10, 4, cols), f32),
            pltpu.SemaphoreType.DMA((5,)),
            pltpu.SemaphoreType.DMA((ROUNDS, 6)),
            pltpu.SemaphoreType.DMA((ROUNDS, 6)),
            pltpu.SemaphoreType.DMA((2, 18)),
            pltpu.SemaphoreType.DMA((2, 18)),
        ],
        compiler_params=pltpu.CompilerParams(collective_id=0, has_side_effects=True),
    )(
        outer_increment.reshape(outer_shape),
        courant,
        obs_column.reshape(observed),
        obs_level.reshape(observed),
        obs_value.reshape(observed),
    )
    state, adjoint, following = pl.pallas_call(
        finish,
        out_shape=(
            jax.ShapeDtypeStruct((levels, rows, cols), f32),
            jax.ShapeDtypeStruct((levels, rows, cols), f32),
            jax.ShapeDtypeStruct(outer_shape, bf16),
        ),
        in_specs=[vmem] * 3,
        out_specs=(hbm,) * 3,
        scratch_shapes=[
            pltpu.VMEM((fine, levels * outer_rows, cols), f32),
            pltpu.VMEM(outer_shape, bf16),
            pltpu.SemaphoreType.DMA((2 + levels,)),
        ],
    )(*[pltpu.with_memory_space_constraint(x, pltpu.VMEM) for x in held])
    return state, adjoint, following.reshape(outer_increment.shape)


def solution(mesh):
    ends = tuple(mesh.shape[a] for a in ("lat", "lon", "lev"))
    block = P("lev", "lat", "lon")
    observed = P(("lat", "lon"))
    return jax.shard_map(
        functools.partial(shards, ends),
        mesh=mesh,
        in_specs=(block, P(None, "lev", "lat", "lon"), observed, observed, observed),
        out_specs=(block, block, block),
        check_vma=False,
    )
```
